256 devices in a mesh: prow: 32 (over z, x), pcol: 8 (over y, core).
Axes of the slice: x: 4, y: 4, z: 8, core: 2. Of those that a mesh axis runs over, the one named last changes fastest.
Arguments:
- cross_cov: float32 [1, 32, 256, 4, 8, 256], P(None, 'prow', None, None, 'pcol'), may hold values from -6 to 6
- left_factor: float32 [1, 32, 256, 512], P(None, 'prow', None, 'pcol'), may hold values from -1 to 3, as said below
- right_factor: float32 [4, 8, 256, 512], P(None, 'pcol', None, 'prow'), may hold values from -1 to 3, as said below
Outputs:
- whitened: float32 [1, 32, 256, 4, 8, 256], P(None, 'prow', None, None, 'pcol')
The draws below stay inside these ranges and needn't reach their ends.
Inputs may be any that keep to these rules, and one draw needn't show every extreme that they name: `left_factor`: the diagonal entries of the diagonal blocks lie between 1.5 and 2. `right_factor`: the diagonal entries of the diagonal blocks lie between 1.5 and 2.
All inputs are finite; a program needn't handle non-finite values.
Results may differ from the reference program's by a relative error of at most 0.0001.
Values sent between devices are 32-bit elements; how exact they have to be, the bound alone decides.
A program may use at most 64 MiB of HBM per device.

```python
import math
import jax
import jax.numpy as jnp
from jax import lax

N = 8192
BS = 256
STEPS = 2
CYC_R = 1
CYC_C = 4
N_PROW = 32
N_PCOL = 8


def panel_draw(key, total_rows):
    first_key, second_key = jax.random.split(jax.random.fold_in(key, 11))
    columns = STEPS * BS
    base = jnp.clip(jax.random.normal(first_key, (total_rows, columns), jnp.float32), -3.0, 3.0) * 0.4
    base = base / math.sqrt(BS)
    diagonal = jax.random.uniform(second_key, (total_rows, 1), jnp.float32, 1.5, 2.0)
    row_ids = jnp.arange(total_rows)[:, None]
    col_ids = jnp.arange(columns)[None, :]
    return jnp.where(row_ids == col_ids, diagonal, base)


def draw_left_factor(key, part):
    return panel_draw(key, N).reshape(CYC_R, N_PROW, BS, STEPS * BS)


def draw_right_factor(key, part):
    return panel_draw(jax.random.fold_in(key, 5), N).reshape(CYC_C, N_PCOL, BS, STEPS * BS)


def steps_of(key, shape, cuts, low, high):
    def one(axis_at, shards_of):
        heights = jax.random.uniform(jax.random.fold_in(jax.random.fold_in(key, 6), axis_at), (shards_of,), jnp.float32, low / len(cuts), high / len(cuts))
        return jnp.repeat(jnp.exp(heights), shape[axis_at] // shards_of).reshape((-1,) + (1,) * (len(shape) - axis_at - 1))

    level = one(*cuts[0])
    for cut in cuts[1:]:
        level = level * one(*cut)
    return level


def noise(key, extent, deviation, most, shards=(), held_as=jnp.bfloat16):
    gain = steps_of(key, extent, shards, -0.22, 0.18) if shards else 1.0
    result = jax.random.normal(key, extent, jnp.float32) * deviation * gain
    return jnp.minimum(jnp.maximum(result, -most), most).astype(held_as)


def setup_inputs(seed: int = 0) -> dict:
    key_of = jax.random.split(jax.random.key(seed), 4)
    return {
        "cross_cov": noise(key_of[0], (CYC_R, N_PROW, BS, CYC_C, N_PCOL, BS), 1.0, 6.0, ((1, 32), (4, 8)), jnp.float32),
        "left_factor": draw_left_factor(jax.random.fold_in(key_of[3], 71), 0),
        "right_factor": draw_right_factor(jax.random.fold_in(key_of[3], 71), 0),
    }


def reference(cross_cov, left_factor, right_factor):
    whole = cross_cov.reshape(N, N)
    left_full = left_factor.reshape(N, STEPS * BS)
    right_full = right_factor.reshape(N, STEPS * BS)
    for block_step in range(STEPS):
        first_row = block_step * BS
        finish = first_row + BS
        solved = jax.scipy.linalg.solve_triangular(left_full[first_row:finish, first_row:finish], whole[first_row:finish], lower=True)
        lower_part = whole[finish:] - jnp.dot(left_full[finish:, first_row:finish], solved, precision=lax.Precision.HIGHEST)
        whole = jnp.concatenate([whole[:first_row], solved, lower_part], 0)
    for block_step in range(STEPS):
        first_col = block_step * BS
        finish = first_col + BS
        solved = jax.scipy.linalg.solve_triangular(right_full[first_col:finish, first_col:finish], whole[:, first_col:finish].T, lower=True).T
        right_part = whole[:, finish:] - jnp.dot(solved, right_full[finish:, first_col:finish].T, precision=lax.Precision.HIGHEST)
        whole = jnp.concatenate([whole[:, :first_col], solved, right_part], 1)
    return whole.reshape(cross_cov.shape)
```

```python
import functools

import jax
import jax.numpy as jnp
from jax import lax
from jax.experimental import pallas as pl
from jax.experimental.pallas import tpu as pltpu
from jax.sharding import PartitionSpec as P

BS = 256
NX = 4
NZ = 8
NY = 4
CUT = 512
MESH = pl.DeviceIdType.MESH


def mm(a, b):
    return jnp.dot(a, b, precision=lax.Precision.HIGHEST, preferred_element_type=jnp.float32)


def tri_inverse(t):
    n, b = t.shape[0], 32
    rows = lax.broadcasted_iota(jnp.int32, (n, n), 0)
    cols = lax.broadcasted_iota(jnp.int32, (n, n), 1)
    t = jnp.where(rows >= cols, t, 0.0)
    same = (rows >> 5) == (cols >> 5)
    wide = (
        (lax.broadcasted_iota(jnp.int32, (b, n), 1) & (b - 1)) == lax.broadcasted_iota(jnp.int32, (b, n), 0)
    ).astype(jnp.float32)
    tall = (
        (lax.broadcasted_iota(jnp.int32, (n, b), 0) & (b - 1)) == lax.broadcasted_iota(jnp.int32, (n, b), 1)
    ).astype(jnp.float32)
    blocks = mm(jnp.where(same, t, 0.0), tall).reshape(n // b, b, b)
    bi = lax.broadcasted_iota(jnp.int32, (n // b, b, b), 1)
    bj = lax.broadcasted_iota(jnp.int32, (n // b, b, b), 2)
    diag = jnp.sum(jnp.where(bi == bj, blocks, 0.0), axis=2, keepdims=True)
    rdiag = 1.0 / diag
    lower = jnp.where(bi > bj, blocks * rdiag, 0.0)
    inv = jnp.where(bi == bj, rdiag, 0.0)
    for j in range(b - 1):
        inv = inv - lower[:, :, j : j + 1] * inv[:, j : j + 1, :]
    full = jnp.where(same, mm(inv.reshape(n, b), wide), 0.0)
    for shift in (5, 6, 7):
        off = ((rows >> (shift + 1)) == (cols >> (shift + 1))) & ((rows >> shift) != (cols >> shift))
        full = full - mm(mm(full, jnp.where(off, t, 0.0)), full)
    return full


def kernel(s_ref, l_ref, r_ref, o_ref, rt, st, tx, lt, yb, send_sem, recv_sem, sc_send, tc_send, sc_recv):
    me = lax.axis_index("prow")
    col = lax.axis_index("pcol")
    z, x = me // NX, me % NX
    y, c = col // 2, col % 2
    own = me

    def at_x(k):
        return (z * NX + (x + k + NX) % NX, col)

    def at_z(k):
        return (((z + k + NZ) % NZ) * NX + x, col)

    def at_y(k):
        return (me, ((y + k + NY) % NY) * 2 + c)

    partner = (me, y * 2 + 1 - c)

    barrier = pltpu.get_barrier_semaphore()
    near = [at_x(1), at_x(-1), at_x(2), at_z(1), at_z(-1), at_y(1), at_y(-1), at_y(2), partner]
    for dev in near:
        pl.semaphore_signal(barrier, inc=1, device_id=dev, device_id_type=MESH)
    for root in range(2):

        @pl.when(me != root)
        def _():
            pl.semaphore_signal(barrier, inc=1, device_id=(root, col), device_id_type=MESH)

    rt[z, x] = r_ref[...].T
    lt[col] = l_ref[...].T
    pl.semaphore_wait(barrier, jnp.where(me < 2, len(near) + NZ * NX - 1, len(near)))

    events = []

    def send(src, dst, dev):
        k = len(events)
        copy = pltpu.make_async_remote_copy(
            src_ref=src, dst_ref=dst, send_sem=send_sem.at[k], recv_sem=recv_sem.at[k], device_id=dev, device_id_type=MESH
        )
        copy.start()
        events.append(copy)
        return copy

    def same(ref, dev):
        return send(ref, ref, dev)

    def s_copy(root, dest):
        return pltpu.make_async_remote_copy(
            src_ref=s_ref.at[pl.ds(dest * 8, 8), :],
            dst_ref=st.at[dest // NX, dest % NX, pl.ds(root * 8, 8), :],
            send_sem=sc_send.at[dest],
            recv_sem=sc_recv.at[root],
            device_id=(dest, col),
            device_id_type=MESH,
        )

    def t_copy(root, k):
        dest = root * 16 + k
        return pltpu.make_async_remote_copy(
            src_ref=lt.at[col, pl.ds((k % 8) * 8, 8), pl.ds((k // 8) * 128, 128)],
            dst_ref=tx.at[col, dest // NX, dest % NX],
            send_sem=tc_send.at[k],
            recv_sem=sc_recv.at[2],
            device_id=(dest, col),
            device_id_type=MESH,
        )

    for root in range(2):

        @pl.when(me == root)
        def _():
            def t_body(k, carry):
                @pl.when(root * 16 + k != root)
                def _():
                    t_copy(root, k).start()

                return carry

            lax.fori_loop(0, 16, t_body, 0)

            def s_body(dest, carry):
                @pl.when(dest != root)
                def _():
                    s_copy(root, dest).start()

                return carry

            lax.fori_loop(0, NZ * NX, s_body, 0)
            st[root // NX, root % NX, root * 8 : root * 8 + 8, :] = s_ref[root * 8 : root * 8 + 8, :]

    @pl.when(me == 0)
    def _():
        tx[col, 0, 0] = lt[col, 0:8, 0:128]

    ca, cb = slice(0, CUT), slice(CUT, 1024)

    class Across:
        def __init__(self, view, plus, minus):
            self.view, self.most = view, {1: plus, -1: minus}
            self.rows = {}

        def first(self):
            self.xs = [same(self.view(z, x), at_x(k)) for k in (1, -1, 2)]

        def step(self, s):
            if s == 1:
                for e in self.xs:
                    e.wait_recv()
            for d in (1, -1):
                if s > 1 and (d, s - 1) in self.rows:
                    self.rows[d, s - 1].wait_recv()
                if s <= self.most[d]:
                    src = (z - d * (s - 1) + NZ) % NZ
                    self.rows[d, s] = same(self.view(src, None), at_z(d))

    class Along:
        def __init__(self, view, plus, minus):
            self.view, self.most = view, {1: plus, -1: minus}
            self.zs, self.xs, self.fs = {}, {}, []

        def to_x(self, key, src, d):
            self.xs[key] = (src, d, {k: same(self.view(src, x), at_x(k)) for k in (1, -1)})

        def first(self):
            for d in (1, -1):
                self.zs[d, 1] = same(self.view(z, x), at_z(d))
            self.to_x((1, 1), z, 1 if self.most[1] == 4 else -1)

        def step(self, s):
            for d in (1, -1):
                if s > 1 and (d, s - 1) in self.zs:
                    self.zs[d, s - 1].wait_recv()
                    src = (z - d * (s - 1) + NZ) % NZ
                    if s <= self.most[d]:
                        self.zs[d, s] = same(self.view(src, x), at_z(d))
                    self.to_x((d, s), src, d if s < 5 else -d)
            for d in (1, -1):
                if (d, s - 1) in self.xs:
                    self.forward((d, s - 1))

        def forward(self, key):
            src, d, sent = self.xs[key]
            sent[1].wait_recv()
            sent[-1].wait_recv()
            self.fs.append(same(self.view(src, (x - d + NX) % NX), at_x(d)))

        def last(self):
            for e in self.fs:
                e.wait_recv()

    def columns(ref, cut):
        def view(zz, xx):
            return ref.at[zz, :, :, cut] if xx is None else ref.at[zz, xx, :, cut]

        return view

    r_a = Across(columns(rt, ca), 4, 3)
    r_b = Along(columns(rt, cb), 4, 3)
    s_a = Across(columns(st, ca), 3, 4)
    s_b = Along(columns(st, cb), 3, 4)
    t_a = Across(lambda zz, xx: tx.at[col, zz] if xx is None else tx.at[col, zz, xx], 4, 3)

    class Panel:
        def __init__(self, ref):
            self.ref = ref

        def first(self):
            self.es = [same(self.ref.at[col], at_y(k)) for k in (1, -1, 2)]
            self.ps = [same(self.ref.at[col], partner)]

        def step(self):
            for k, e in zip((1, -1, 2), self.es):
                e.wait_recv()
                self.ps.append(same(self.ref.at[((y - k + NY) % NY) * 2 + c], partner))

        def last(self):
            for e in self.ps:
                e.wait_recv()

    l_p, t_p = Panel(lt), Panel(tx)

    l_p.first()
    r_a.first()
    r_b.first()

    @pl.when(me != 0)
    def _():
        t_copy(0, 0).wait_recv()

    t_a.first()
    r_a.step(1)
    l_p.step()
    t_a.step(1)
    r_b.step(2)
    r_a.step(2)
    t_a.step(2)

    @pl.when(me != 0)
    def _():
        s_copy(0, 0).wait_recv()

    @pl.when(me != 1)
    def _():
        s_copy(1, 0).wait_recv()

    s_a.first()
    s_b.first()
    r_b.step(3)
    t_a.step(3)
    r_a.step(3)
    s_a.step(1)
    s_b.step(2)
    t_a.step(4)
    r_b.step(4)
    r_a.step(4)
    t_a.step(5)
    t_p.first()
    s_a.step(2)
    s_b.step(3)
    r_b.step(5)
    r_a.step(5)
    t_p.step()
    s_a.step(3)
    s_b.step(4)
    r_b.step(6)
    s_a.step(4)
    s_b.step(5)
    r_b.last()
    s_a.step(5)
    s_b.step(6)
    s_b.last()
    l_p.last()
    t_p.last()

    def panel_of(root):
        halves = [tx[:, 4 * root + 2 * h : 4 * root + 2 * h + 2].reshape(512, 128) for h in range(2)]
        return jnp.concatenate(halves, axis=1)

    left0 = panel_of(0)
    left1 = panel_of(1)
    inv0 = tri_inverse(left0[0:BS].T)
    inv1 = tri_inverse(left1[BS:].T)
    t10 = left1[0:BS].T
    mine = lt[...].reshape(512, BS).T
    ri = lax.broadcasted_iota(jnp.int32, (BS, 512), 0)
    ci = lax.broadcasted_iota(jnp.int32, (BS, 512), 1)
    unit = jnp.where(ci == ri + me * BS, -1.0, 0.0)
    a = jnp.where(me < 2, unit, mine)
    w1 = mm(a[:, BS:], inv1)
    w0 = mm(a[:, :BS] - mm(w1, t10), inv0)
    base = jnp.where(me < 2, 0.0, s_ref[...])
    o_ref[...] = base - mm(w0, st[:, :, 0:8, :].reshape(BS, 1024)) - mm(w1, st[:, :, 8:16, :].reshape(BS, 1024))

    y_up = [
        pltpu.make_async_remote_copy(
            src_ref=yb.at[c],
            dst_ref=yb.at[c],
            send_sem=send_sem.at[len(events) + k],
            recv_sem=recv_sem.at[len(events) + 3],
            device_id=(me, k * 2 + c),
            device_id_type=MESH,
        )
        for k in (1, 2, 3)
    ]
    y_over = pltpu.make_async_remote_copy(
        src_ref=yb.at[c],
        dst_ref=yb.at[c],
        send_sem=send_sem.at[len(events) + 4],
        recv_sem=recv_sem.at[len(events) + 4],
        device_id=partner,
        device_id_type=MESH,
    )

    @pl.when(y == 0)
    def _():
        block = rt[pl.ds(4 * c, 4), :, :, 0:BS].reshape(BS, BS)
        yinv = tri_inverse(block.T).T

        @pl.when(c == 1)
        def _():
            y_over.wait_recv()
            o_ref[:, 0:BS] = o_ref[:, 0:BS] - mm(yb[0], rt[0:4, :, :, 0:BS].reshape(BS, BS))

        yb[c] = mm(o_ref[:, 0:BS], yinv)
        y_over.start()
        for e in y_up:
            e.start()

    @pl.when(y != 0)
    def _():
        y_up[0].wait_recv()
        y_over.start()

    @pl.when((y != 0) | (c == 0))
    def _():
        y_over.wait_recv()

    def right(cut):
        return o_ref[:, cut] - mm(yb[0], rt[0:4, :, :, cut].reshape(BS, -1)) - mm(yb[1], rt[4:8, :, :, cut].reshape(BS, -1))

    o_ref[:, 256:1024] = right(slice(256, 1024))

    @pl.when(y == 0)
    def _():
        o_ref[:, 0:BS] = yb[c]

    @pl.when(y != 0)
    def _():
        o_ref[:, 0:BS] = right(slice(0, 256))

    for e in events:
        e.wait_send()
    y_over.wait_send()

    @pl.when(y == 0)
    def _():
        for e in y_up:
            e.wait_send()

    for root in range(2):

        @pl.when(me == root)
        def _():
            def t_body(k, carry):
                @pl.when(root * 16 + k != root)
                def _():
                    t_copy(root, k).wait_send()

                return carry

            lax.fori_loop(0, 16, t_body, 0)

            def s_body(dest, carry):
                @pl.when(dest != root)
                def _():
                    s_copy(root, dest).wait_send()

                return carry

            lax.fori_loop(0, NZ * NX, s_body, 0)


N_EVENTS = 120


def shards(cross_cov, left_factor, right_factor):
    f32 = jnp.float32
    out = pl.pallas_call(
        kernel,
        out_shape=jax.ShapeDtypeStruct((BS, 1024), f32),
        in_specs=[pl.BlockSpec(memory_space=pltpu.VMEM)] * 3,
        out_specs=pl.BlockSpec(memory_space=pltpu.VMEM),
        scratch_shapes=[
            pltpu.VMEM((NZ, NX, 16, 1024), f32),
            pltpu.VMEM((NZ, NX, 16, 1024), f32),
            pltpu.VMEM((8, NZ, NX, 8, 128), f32),
            pltpu.VMEM((8, 64, 256), f32),
            pltpu.VMEM((2, BS, BS), f32),
            pltpu.SemaphoreType.DMA((N_EVENTS,)),
            pltpu.SemaphoreType.DMA((N_EVENTS,)),
            pltpu.SemaphoreType.DMA((NZ * NX,)),
            pltpu.SemaphoreType.DMA((16,)),
            pltpu.SemaphoreType.DMA((3,)),
        ],
        compiler_params=pltpu.CompilerParams(collective_id=0, has_side_effects=True, vmem_limit_bytes=60 * 1024 * 1024),
    )(
        cross_cov.reshape(BS, 1024),
        left_factor.reshape(BS, 64),
        right_factor.reshape(1024, 16),
    )
    return out.reshape(cross_cov.shape)


def solution(mesh):
    return jax.shard_map(
        shards,
        mesh=mesh,
        in_specs=(
            P(None, "prow", None, None, "pcol", None),
            P(None, "prow", None, "pcol"),
            P(None, "pcol", None, "prow"),
        ),
        out_specs=P(None, "prow", None, None, "pcol", None),
        check_vma=False,
    )
```

```python
import functools

import jax
import jax.numpy as jnp
from jax import lax
from jax.experimental import pallas as pl
from jax.experimental.pallas import tpu as pltpu
from jax.sharding import PartitionSpec as P

BS = 256
NX = 4
NZ = 8
NY = 4
CUT = 512
MESH = pl.DeviceIdType.MESH


def mm(a, b):
    return jnp.dot(a, b, precision=lax.Precision.HIGHEST, preferred_element_type=jnp.float32)


def tri_inverse(t):
    n, b = t.shape[0], 32
    rows = lax.broadcasted_iota(jnp.int32, (n, n), 0)
    cols = lax.broadcasted_iota(jnp.int32, (n, n), 1)
    t = jnp.where(rows >= cols, t, 0.0)
    same = (rows >> 5) == (cols >> 5)
    wide = (
        (lax.broadcasted_iota(jnp.int32, (b, n), 1) & (b - 1)) == lax.broadcasted_iota(jnp.int32, (b, n), 0)
    ).astype(jnp.float32)
    tall = (
        (lax.broadcasted_iota(jnp.int32, (n, b), 0) & (b - 1)) == lax.broadcasted_iota(jnp.int32, (n, b), 1)
    ).astype(jnp.float32)
    blocks = mm(jnp.where(same, t, 0.0), tall).reshape(n // b, b, b)
    bi = lax.broadcasted_iota(jnp.int32, (n // b, b, b), 1)
    bj = lax.broadcasted_iota(jnp.int32, (n // b, b, b), 2)
    diag = jnp.sum(jnp.where(bi == bj, blocks, 0.0), axis=2, keepdims=True)
    rdiag = 1.0 / diag
    lower = jnp.where(bi > bj, blocks * rdiag, 0.0)
    inv = jnp.where(bi == bj, rdiag, 0.0)
    for j in range(b - 1):
        inv = inv - lower[:, :, j : j + 1] * inv[:, j : j + 1, :]
    full = jnp.where(same, mm(inv.reshape(n, b), wide), 0.0)
    for shift in (5, 6, 7):
        off = ((rows >> (shift + 1)) == (cols >> (shift + 1))) & ((rows >> shift) != (cols >> shift))
        full = full - mm(mm(full, jnp.where(off, t, 0.0)), full)
    return full


def kernel(s_hbm, l_ref, r_ref, o_hbm, s_ref, o_ref, rt, st, tx, lt, yb, io_sem, send_sem, recv_sem, sc_send, tc_send, sc_recv):
    me = lax.axis_index("prow")
    col = lax.axis_index("pcol")
    z, x = me // NX, me % NX
    y, c = col // 2, col % 2
    own = me

    def at_x(k):
        return (z * NX + (x + k + NX) % NX, col)

    def at_z(k):
        return (((z + k + NZ) % NZ) * NX + x, col)

    def at_y(k):
        return (me, ((y + k + NY) % NY) * 2 + c)

    partner = (me, y * 2 + 1 - c)

    s_in = [
        pltpu.make_async_copy(s_hbm.at[:, h, :], s_ref.at[:, h * 128 : (h + 1) * 128], io_sem.at[h]) for h in range(8)
    ]
    o_out = [
        pltpu.make_async_copy(o_ref.at[:, h * 128 : (h + 1) * 128], o_hbm.at[:, h, :], io_sem.at[8 + h]) for h in range(8)
    ]
    for e in s_in:
        e.start()
    barrier = pltpu.get_barrier_semaphore()
    near = [at_x(1), at_x(-1), at_x(2), at_z(1), at_z(-1), at_y(1), at_y(-1), at_y(2), partner]
    for dev in near:
        pl.semaphore_signal(barrier, inc=1, device_id=dev, device_id_type=MESH)
    for root in range(2):

        @pl.when(me != root)
        def _():
            pl.semaphore_signal(barrier, inc=1, device_id=(root, col), device_id_type=MESH)

    rt[z, x] = r_ref[...]
    lt[col] = l_ref[...]
    pl.semaphore_wait(barrier, jnp.where(me < 2, len(near) + NZ * NX - 1, len(near)))

    for e in s_in:
        e.wait()
    events = []

    def send(src, dst, dev):
        k = len(events)
        copy = pltpu.make_async_remote_copy(
            src_ref=src, dst_ref=dst, send_sem=send_sem.at[k], recv_sem=recv_sem.at[k], device_id=dev, device_id_type=MESH
        )
        copy.start()
        events.append(copy)
        return copy

    def same(ref, dev):
        return send(ref, ref, dev)

    def s_copy(root, dest):
        return pltpu.make_async_remote_copy(
            src_ref=s_ref.at[pl.ds(dest * 8, 8), :],
            dst_ref=st.at[dest // NX, dest % NX, pl.ds(root * 8, 8), :],
            send_sem=sc_send.at[dest],
            recv_sem=sc_recv.at[root],
            device_id=(dest, col),
            device_id_type=MESH,
        )

    def t_copy(root, k):
        dest = root * 16 + k
        return pltpu.make_async_remote_copy(
            src_ref=lt.at[col, pl.ds((k % 8) * 8, 8), pl.ds((k // 8) * 128, 128)],
            dst_ref=tx.at[col, dest // NX, dest % NX],
            send_sem=tc_send.at[k],
            recv_sem=sc_recv.at[2],
            device_id=(dest, col),
            device_id_type=MESH,
        )

    for root in range(2):

        @pl.when(me == root)
        def _():
            def t_body(k, carry):
                @pl.when(root * 16 + k != root)
                def _():
                    t_copy(root, k).start()

                return carry

            lax.fori_loop(0, 16, t_body, 0)

            def s_body(dest, carry):
                @pl.when(dest != root)
                def _():
                    s_copy(root, dest).start()

                return carry

            lax.fori_loop(0, NZ * NX, s_body, 0)
            st[root // NX, root % NX, root * 8 : root * 8 + 8, :] = s_ref[root * 8 : root * 8 + 8, :]

    @pl.when(me == 0)
    def _():
        tx[col, 0, 0] = lt[col, 0:8, 0:128]


    class Across:
        def __init__(self, view, plus, minus):
            self.view, self.most = view, {1: plus, -1: minus}
            self.rows = {}

        def first(self):
            self.xs = [same(self.view(z, x), at_x(k)) for k in (1, -1, 2)]

        def step(self, s):
            if s == 1:
                for e in self.xs:
                    e.wait_recv()
            for d in (1, -1):
                if s > 1 and (d, s - 1) in self.rows:
                    self.rows[d, s - 1].wait_recv()
                if s <= self.most[d]:
                    src = (z - d * (s - 1) + NZ) % NZ
                    self.rows[d, s] = same(self.view(src, None), at_z(d))

    class Along:
        def __init__(self, view, plus, minus):
            self.view, self.most = view, {1: plus, -1: minus}
            self.zs, self.xs, self.fs = {}, {}, []

        def to_x(self, key, src, d):
            self.xs[key] = (src, d, {k: same(self.view(src, x), at_x(k)) for k in (1, -1)})

        def first(self):
            for d in (1, -1):
                self.zs[d, 1] = same(self.view(z, x), at_z(d))
            self.to_x((1, 1), z, 1 if self.most[1] == 4 else -1)

        def step(self, s):
            for d in (1, -1):
                if s > 1 and (d, s - 1) in self.zs:
                    self.zs[d, s - 1].wait_recv()
                    src = (z - d * (s - 1) + NZ) % NZ
                    if s <= self.most[d]:
                        self.zs[d, s] = same(self.view(src, x), at_z(d))
                    self.to_x((d, s), src, d if s < 5 else -d)
            for d in (1, -1):
                if (d, s - 1) in self.xs:
                    self.forward((d, s - 1))

        def forward(self, key):
            src, d, sent = self.xs[key]
            sent[1].wait_recv()
            sent[-1].wait_recv()
            self.fs.append(same(self.view(src, (x - d + NX) % NX), at_x(d)))

        def last(self):
            for e in self.fs:
                e.wait_recv()

    def blocks(first):
        def view(zz, xx):
            return rt.at[zz, :, first : first + 2] if xx is None else rt.at[zz, xx, first : first + 2]

        return view

    def columns(first):
        cut = slice(first, first + 512)

        def view(zz, xx):
            return st.at[zz, :, :, cut] if xx is None else st.at[zz, xx, :, cut]

        return view

    r_a = Across(blocks(0), 4, 3)
    r_b = Along(blocks(2), 4, 3)
    s_a = Across(columns(0), 3, 4)
    s_b = Along(columns(512), 3, 4)
    t_a = Across(lambda zz, xx: tx.at[col, zz] if xx is None else tx.at[col, zz, xx], 4, 3)

    class Panel:
        def __init__(self, ref):
            self.ref = ref

        def first(self):
            self.es = [same(self.ref.at[col], at_y(k)) for k in (1, -1, 2)]
            self.ps = [same(self.ref.at[col], partner)]

        def step(self):
            for k, e in zip((1, -1, 2), self.es):
                e.wait_recv()
                self.ps.append(same(self.ref.at[((y - k + NY) % NY) * 2 + c], partner))

        def last(self):
            for e in self.ps:
                e.wait_recv()

    l_p, t_p = Panel(lt), Panel(tx)

    l_p.first()
    r_a.first()
    r_b.first()

    @pl.when(me != 0)
    def _():
        t_copy(0, 0).wait_recv()

    t_a.first()
    r_a.step(1)
    l_p.step()
    t_a.step(1)
    r_b.step(2)
    r_a.step(2)
    t_a.step(2)

    @pl.when(me != 0)
    def _():
        s_copy(0, 0).wait_recv()

    @pl.when(me != 1)
    def _():
        s_copy(1, 0).wait_recv()

    s_a.first()
    s_b.first()
    r_b.step(3)
    t_a.step(3)
    r_a.step(3)
    s_a.step(1)
    s_b.step(2)
    t_a.step(4)
    r_b.step(4)
    r_a.step(4)
    t_a.step(5)
    t_p.first()
    s_a.step(2)
    s_b.step(3)
    r_b.step(5)
    r_a.step(5)
    t_p.step()
    s_a.step(3)
    s_b.step(4)
    r_b.step(6)
    s_a.step(4)
    s_b.step(5)
    r_b.last()
    s_a.step(5)
    s_b.step(6)
    s_b.last()
    l_p.last()
    t_p.last()

    def panel_of(root):
        halves = [tx[:, 4 * root + 2 * h : 4 * root + 2 * h + 2].reshape(512, 128) for h in range(2)]
        return jnp.concatenate(halves, axis=1)

    left0 = panel_of(0)
    left1 = panel_of(1)
    inv0 = tri_inverse(left0[0:BS].T)
    inv1 = tri_inverse(left1[BS:].T)
    t10 = left1[0:BS].T
    mine = lt[...].reshape(512, BS).T
    ri = lax.broadcasted_iota(jnp.int32, (BS, 512), 0)
    ci = lax.broadcasted_iota(jnp.int32, (BS, 512), 1)
    unit = jnp.where(ci == ri + me * BS, -1.0, 0.0)
    a = jnp.where(me < 2, unit, mine)
    w1 = mm(a[:, BS:], inv1)
    w0 = mm(a[:, :BS] - mm(w1, t10), inv0)
    base = jnp.where(me < 2, 0.0, s_ref[...])
    o_ref[...] = base - mm(w0, st[:, :, 0:8, :].reshape(BS, 1024)) - mm(w1, st[:, :, 8:16, :].reshape(BS, 1024))

    y_up = [
        pltpu.make_async_remote_copy(
            src_ref=yb.at[c],
            dst_ref=yb.at[c],
            send_sem=send_sem.at[len(events) + k],
            recv_sem=recv_sem.at[len(events) + 3],
            device_id=(me, k * 2 + c),
            device_id_type=MESH,
        )
        for k in (1, 2, 3)
    ]
    y_over = pltpu.make_async_remote_copy(
        src_ref=yb.at[c],
        dst_ref=yb.at[c],
        send_sem=send_sem.at[len(events) + 4],
        recv_sem=recv_sem.at[len(events) + 4],
        device_id=partner,
        device_id_type=MESH,
    )

    @pl.when(y == 0)
    def _():
        block = rt[pl.ds(4 * c, 4), :, 0].reshape(BS, BS)
        yinv = tri_inverse(block.T).T

        @pl.when(c == 1)
        def _():
            y_over.wait_recv()
            o_ref[:, 0:BS] = o_ref[:, 0:BS] - mm(yb[0], rt[0:4, :, 0].reshape(BS, BS))

        yb[c] = mm(o_ref[:, 0:BS], yinv)
        y_over.start()
        for e in y_up:
            e.start()

    @pl.when(y != 0)
    def _():
        y_up[0].wait_recv()
        y_over.start()

    @pl.when((y != 0) | (c == 0))
    def _():
        y_over.wait_recv()

    def right(d):
        cut = slice(d * BS, (d + 1) * BS)
        o_ref[:, cut] = (
            o_ref[:, cut] - mm(yb[0], rt[0:4, :, d].reshape(BS, BS)) - mm(yb[1], rt[4:8, :, d].reshape(BS, BS))
        )

    for d in (1, 2, 3):
        right(d)
        o_out[2 * d].start()
        o_out[2 * d + 1].start()

    @pl.when(y == 0)
    def _():
        o_ref[:, 0:BS] = yb[c]

    @pl.when(y != 0)
    def _():
        right(0)

    o_out[0].start()
    o_out[1].start()

    for e in events:
        e.wait_send()
    y_over.wait_send()

    @pl.when(y == 0)
    def _():
        for e in y_up:
            e.wait_send()

    for root in range(2):

        @pl.when(me == root)
        def _():
            def t_body(k, carry):
                @pl.when(root * 16 + k != root)
                def _():
                    t_copy(root, k).wait_send()

                return carry

            lax.fori_loop(0, 16, t_body, 0)

            def s_body(dest, carry):
                @pl.when(dest != root)
                def _():
                    s_copy(root, dest).wait_send()

                return carry

            lax.fori_loop(0, NZ * NX, s_body, 0)

    for e in o_out:
        e.wait()


N_EVENTS = 120


def shards(cross_cov, left_factor, right_factor):
    f32 = jnp.float32
    out = pl.pallas_call(
        kernel,
        out_shape=jax.ShapeDtypeStruct((BS, 8, 128), f32),
        in_specs=[
            pl.BlockSpec(memory_space=pl.ANY),
            pl.BlockSpec(memory_space=pltpu.VMEM),
            pl.BlockSpec(memory_space=pltpu.VMEM),
        ],
        out_specs=pl.BlockSpec(memory_space=pl.ANY),
        scratch_shapes=[
            pltpu.VMEM((BS, 1024), f32),
            pltpu.VMEM((BS, 1024), f32),
            pltpu.VMEM((NZ, NX, 4, 16, BS), f32),
            pltpu.VMEM((NZ, NX, 16, 1024), f32),
            pltpu.VMEM((8, NZ, NX, 8, 128), f32),
            pltpu.VMEM((8, 64, 256), f32),
            pltpu.VMEM((2, BS, BS), f32),
            pltpu.SemaphoreType.DMA((16,)),
            pltpu.SemaphoreType.DMA((N_EVENTS,)),
            pltpu.SemaphoreType.DMA((N_EVENTS,)),
            pltpu.SemaphoreType.DMA((NZ * NX,)),
            pltpu.SemaphoreType.DMA((16,)),
            pltpu.SemaphoreType.DMA((3,)),
        ],
        compiler_params=pltpu.CompilerParams(collective_id=0, has_side_effects=True, vmem_limit_bytes=60 * 1024 * 1024),
    )(
        cross_cov.reshape(BS, 8, 128),
        left_factor.reshape(BS, 64).T,
        jnp.swapaxes(right_factor.reshape(4, BS, 16), 1, 2),
    )
    return out.reshape(cross_cov.shape)


def solution(mesh):
    return jax.shard_map(
        shards,
        mesh=mesh,
        in_specs=(
            P(None, "prow", None, None, "pcol", None),
            P(None, "prow", None, "pcol"),
            P(None, "pcol", None, "prow"),
        ),
        out_specs=P(None, "prow", None, None, "pcol", None),
        check_vma=False,
    )
```

```python
import functools

import jax
import jax.numpy as jnp
from jax import lax
from jax.experimental import pallas as pl
from jax.experimental.pallas import tpu as pltpu
from jax.sharding import PartitionSpec as P

BS = 256
NX = 4
NZ = 8
NY = 4
R_CUT = 2
MESH = pl.DeviceIdType.MESH


def mm(a, b):
    return jnp.dot(a, b, precision=lax.Precision.HIGHEST, preferred_element_type=jnp.float32)


def inverse_stages(ts, result):
    n, b = ts[0].shape[0], 32
    m = n // b
    rows = lax.broadcasted_iota(jnp.int32, (n, n), 0)
    cols = lax.broadcasted_iota(jnp.int32, (n, n), 1)
    same = (rows >> 5) == (cols >> 5)
    wide = (
        (lax.broadcasted_iota(jnp.int32, (b, n), 1) & (b - 1)) == lax.broadcasted_iota(jnp.int32, (b, n), 0)
    ).astype(jnp.float32)
    tall = (
        (lax.broadcasted_iota(jnp.int32, (n, b), 0) & (b - 1)) == lax.broadcasted_iota(jnp.int32, (n, b), 1)
    ).astype(jnp.float32)
    ts = [jnp.where(rows >= cols, t, 0.0) for t in ts]
    blocks = jnp.concatenate([mm(jnp.where(same, t, 0.0), tall).reshape(m, b, b) for t in ts], axis=0)
    bi = lax.broadcasted_iota(jnp.int32, blocks.shape, 1)
    bj = lax.broadcasted_iota(jnp.int32, blocks.shape, 2)
    diag = jnp.sum(jnp.where(bi == bj, blocks, 0.0), axis=2, keepdims=True)
    rdiag = 1.0 / diag
    lower = jnp.where(bi > bj, blocks * rdiag, 0.0)
    inv = jnp.where(bi == bj, rdiag, 0.0)
    yield
    for j in range(b - 1):
        inv = inv - lower[:, :, j : j + 1] * inv[:, j : j + 1, :]
        if j == b // 2:
            yield
    fulls = [jnp.where(same, mm(inv[k * m : k * m + m].reshape(n, b), wide), 0.0) for k in range(len(ts))]
    yield
    for shift in (5, 6, 7):
        off = ((rows >> (shift + 1)) == (cols >> (shift + 1))) & ((rows >> shift) != (cols >> shift))
        parts = [mm(full, jnp.where(off, t, 0.0)) for full, t in zip(fulls, ts)]
        fulls = [full - mm(part, full) for full, part in zip(fulls, parts)]
        yield
    result.extend(fulls)


def kernel(s_hbm, l_ref, r_ref, o_hbm, s_ref, o_ref, rt, st, tx, lt, yb, io_sem, send_sem, recv_sem, sh_send, s_send, s_recv, t_send, t_recv, y_send, y_recv):
    me = lax.axis_index("prow")
    col = lax.axis_index("pcol")
    z, x = me // NX, me % NX
    y, c = col // 2, col % 2

    def at_x(k):
        return (z * NX + (x + k + NX) % NX, col)

    def at_z(k):
        return (((z + k + NZ) % NZ) * NX + x, col)

    def at_y(k):
        return (me, ((y + k + NY) % NY) * 2 + c)

    partner = (me, y * 2 + 1 - c)

    s_in = [
        pltpu.make_async_copy(s_hbm.at[:, h, :], s_ref.at[:, h * 128 : (h + 1) * 128], io_sem.at[h]) for h in range(8)
    ]
    o_out = [
        pltpu.make_async_copy(o_ref.at[:, h * 128 : (h + 1) * 128], o_hbm.at[:, h, :], io_sem.at[8 + h]) for h in range(8)
    ]
    for e in s_in:
        e.start()
    barrier = pltpu.get_barrier_semaphore()
    near = [at_x(1), at_x(-1), at_x(2), at_z(1), at_z(-1), at_y(1), at_y(-1), at_y(2), partner]
    for dev in near:
        pl.semaphore_signal(barrier, inc=1, device_id=dev, device_id_type=MESH)
    rt[z, x] = r_ref[...]
    lt[col] = l_ref[...]
    pl.semaphore_wait(barrier, len(near))

    for e in s_in:
        e.wait()
    for root in range(2):

        @pl.when(me == root)
        def _():
            st[root, root * 4 : root * 4 + 4] = s_ref[:, root * BS : (root + 1) * BS].reshape(4, 64, BS)
            tx[col, root, root * 16 : root * 16 + 16] = l_ref[root * 16 : root * 16 + 16]

    events = []

    def send(src, dst, dev):
        k = len(events)
        copy = pltpu.make_async_remote_copy(
            src_ref=src, dst_ref=dst, send_sem=send_sem.at[k], recv_sem=recv_sem.at[k], device_id=dev, device_id_type=MESH
        )
        copy.start()
        events.append(copy)
        return copy

    def same(ref, dev):
        return send(ref, ref, dev)

    def remote(src, dst, ssem, rsem, dev):
        return pltpu.make_async_remote_copy(
            src_ref=src, dst_ref=dst, send_sem=ssem, recv_sem=rsem, device_id=dev, device_id_type=MESH
        )

    dist = jnp.where(z <= NZ // 2, z, NZ - z)
    zdir = jnp.where(z <= NZ // 2, 1, -1)
    passes_on = ((z >= 1) & (z <= 3)) | (z >= 6)

    def s_share(root, k, d):
        return remote(
            s_ref.at[pl.ds(k * 64, 64), pl.ds(d * BS, BS)],
            st.at[d, root * 4 + k],
            sh_send.at[k * 4 + d],
            s_recv.at[0, root * 4 + k],
            (d, col),
        )

    def s_along(k, d, which):
        return remote(st.at[x, k], st.at[x, k], s_send.at[which, k], s_recv.at[0, k], at_z(d))

    def s_across(k, which):
        return remote(st.at[x, k], st.at[x, k], s_send.at[2 + which, k], s_recv.at[1 + which, k], at_x(1 - 2 * which))

    def s_over(k):
        d = 1 - 2 * (k % 2)
        part = st.at[(x - d + NX) % NX, k]
        return remote(part, part, s_send.at[4, k], s_recv.at[3, k], at_x(d))

    def s_slot(j):
        turn = j - dist

        @pl.when((turn >= 0) & (turn < 8))
        def _():
            k = turn // 2 + 4 * (turn % 2)

            @pl.when((z != 0) | (x != k // 4))
            def _():
                s_along(k, 1, 0).wait_recv()

            @pl.when(z == 0)
            def _():
                s_along(k, 1, 0).start()
                s_along(k, -1, 1).start()

            @pl.when(passes_on)
            def _():
                s_along(k, zdir, 0).start()

            s_across(k, 0).start()
            s_across(k, 1).start()

        @pl.when((turn >= 1) & (turn < 9))
        def _():
            k = (turn - 1) // 2 + 4 * ((turn - 1) % 2)
            s_across(k, 0).wait_recv()
            s_across(k, 1).wait_recv()
            s_over(k).start()

    def s_end():
        for k in range(8):
            s_over(k).wait_recv()

    def s_sent():
        @pl.when((z == 0) | passes_on)
        def _():
            for k in range(8):
                s_along(k, 1, 0).wait_send()

        @pl.when(z == 0)
        def _():
            for k in range(8):
                s_along(k, -1, 1).wait_send()

        for k in range(8):
            s_across(k, 0).wait_send()
            s_across(k, 1).wait_send()
            s_over(k).wait_send()

    def t_share(root, d):
        return remote(
            l_ref.at[pl.ds(d * 16, 16)],
            tx.at[col, root, pl.ds(d * 16, 16)],
            t_send.at[d],
            t_recv.at[root],
            (d, col),
        )

    quarter = tx.at[col, :, pl.ds(x * 16, 16)]
    t_along = [remote(quarter, quarter, t_send.at[4 + w], t_recv.at[2], at_z(d)) for w, d in enumerate((1, -1, zdir))]
    t_across = [remote(quarter, quarter, t_send.at[7 + w], t_recv.at[3 + w], at_x(d)) for w, d in enumerate((1, -1, 2))]
    t_up = [remote(tx.at[col], tx.at[col], t_send.at[10 + w], t_recv.at[6 + w], at_y(d)) for w, d in enumerate((1, -1, 2))]

    def t_over(w):
        part = tx.at[((y - (0, 1, -1, 2)[w] + NY) % NY) * 2 + c]
        return remote(part, part, t_send.at[13 + w], t_recv.at[9 + w], partner)

    def t_slot(n):
        @pl.when(dist == n)
        def _():
            if n == 0:
                for root in range(2):

                    @pl.when(x != root)
                    def _():
                        t_share(root, x).wait_recv()

                t_along[0].start()
                t_along[1].start()
            else:
                t_along[2].wait_recv()

                @pl.when(passes_on)
                def _():
                    t_along[2].start()

            for e in t_across:
                e.start()

        @pl.when(dist == n - 1)
        def _():
            for e in t_across:
                e.wait_recv()
            for e in t_up:
                e.start()
            t_over(0).start()

    def t_step():
        for w in range(3):
            t_up[w].wait_recv()
            t_over(w + 1).start()

    def t_end():
        for w in range(4):
            t_over(w).wait_recv()

    def t_sent():
        @pl.when(z == 0)
        def _():
            t_along[0].wait_send()
            t_along[1].wait_send()

        @pl.when(passes_on)
        def _():
            t_along[2].wait_send()

        for e in t_across + t_up + [t_over(w) for w in range(4)]:
            e.wait_send()

    def t_shares():
        for root in range(2):

            @pl.when(me == root)
            def _():
                for d in range(NX):
                    if d != root:
                        t_share(root, d).start()

    def s_shares(k):
        for root in range(2):

            @pl.when(me == root)
            def _():
                for d in range(NX):
                    if d != root:
                        s_share(root, k, d).start()

    def shares_sent():
        for root in range(2):

            @pl.when(me == root)
            def _():
                for d in range(NX):
                    if d != root:
                        t_share(root, d).wait_send()
                        for k in range(4):
                            s_share(root, k, d).wait_send()

    class Across:
        def __init__(self, view, plus, minus):
            self.view, self.most = view, {1: plus, -1: minus}
            self.sent = {}

        def on(self, d, s, off):
            src = (z - d * (s - 1) + NZ) % NZ
            self.sent[d, s, off] = same(self.view(src, (x + off + NX) % NX), at_z(d))

        def first(self):
            self.xs = [same(self.view(z, x), at_x(k)) for k in (1, -1, 2)]
            for d in (1, -1):
                self.on(d, 1, 0)

        def step(self, s):
            if s == 1:
                for e, k in zip(self.xs, (1, -1, 2)):
                    e.wait_recv()
                    for d in (1, -1):
                        self.on(d, 1, -k)
                return
            for off in (0, -1, 1, -2):
                for d in (1, -1):
                    if (d, s - 1, off) in self.sent:
                        self.sent[d, s - 1, off].wait_recv()
                    if s <= self.most[d]:
                        self.on(d, s, off)

    class Along:
        def __init__(self, view, plus, minus):
            self.view, self.most = view, {1: plus, -1: minus}
            self.zs, self.xs, self.fs = {}, {}, []

        def to_x(self, key, src, d):
            self.xs[key] = (src, d, {k: same(self.view(src, x), at_x(k)) for k in (1, -1)})

        def first(self):
            for d in (1, -1):
                self.zs[d, 1] = same(self.view(z, x), at_z(d))
            self.to_x((1, 1), z, 1 if self.most[1] == 4 else -1)

        def step(self, s):
            for d in (1, -1):
                if s > 1 and (d, s - 1) in self.zs:
                    self.zs[d, s - 1].wait_recv()
                    src = (z - d * (s - 1) + NZ) % NZ
                    if s <= self.most[d]:
                        self.zs[d, s] = same(self.view(src, x), at_z(d))
                    self.to_x((d, s), src, d if s < 5 else -d)
            for d in (1, -1):
                if (d, s - 1) in self.xs:
                    self.forward((d, s - 1))

        def forward(self, key):
            src, d, sent = self.xs[key]
            sent[1].wait_recv()
            sent[-1].wait_recv()
            self.fs.append(same(self.view(src, (x - d + NX) % NX), at_x(d)))

        def last(self):
            for e in self.fs:
                e.wait_recv()

    def blocks(first, number):
        def view(zz, xx):
            return rt.at[zz, xx, first : first + number]

        return view

    r_a = Across(blocks(0, R_CUT), 4, 3)
    r_b = Along(blocks(R_CUT, 4 - R_CUT), 4, 3)

    class Panel:
        def __init__(self, ref):
            self.ref = ref

        def first(self):
            self.es = [same(self.ref.at[col], at_y(k)) for k in (1, -1, 2)]
            self.ps = [same(self.ref.at[col], partner)]

        def step(self):
            for k, e in zip((1, -1, 2), self.es):
                e.wait_recv()
                self.ps.append(same(self.ref.at[((y - k + NY) % NY) * 2 + c], partner))

        def last(self):
            for e in self.ps:
                e.wait_recv()

    l_p = Panel(lt)

    def panel_of(root):
        return tx[:, root].reshape(512, BS)

    t_shares()
    r_a.first()
    r_b.first()
    l_p.first()
    t_slot(0)
    s_shares(0)
    r_a.step(1)
    r_b.step(2)
    s_shares(1)
    t_slot(1)
    s_slot(0)
    s_shares(2)
    r_b.step(3)
    r_a.step(2)
    s_shares(3)
    t_slot(2)
    s_slot(1)
    r_b.step(4)
    t_slot(3)
    s_slot(2)
    r_a.step(3)
    t_slot(4)
    r_b.step(5)
    s_slot(3)
    t_slot(5)
    r_a.step(4)
    r_b.step(6)
    l_p.step()
    t_step()
    s_slot(4)
    l_p.last()
    t_end()
    left0 = panel_of(0)
    left1 = panel_of(1)
    x_inv = []
    x_stages = inverse_stages([left0[0:BS].T, left1[BS:].T], x_inv)
    next(x_stages)
    r_a.step(5)
    y_inv = []
    y_stages = inverse_stages([rt[pl.ds(4 * c, 4), :, 0].reshape(BS, BS).T], y_inv)
    s_slot(5)
    next(x_stages)
    next(y_stages)
    s_slot(6)
    next(x_stages)
    s_slot(7)
    next(x_stages)
    next(y_stages)
    s_slot(8)
    next(x_stages)
    next(y_stages)
    s_slot(9)
    next(x_stages)
    next(y_stages)
    s_slot(10)
    for _ in x_stages:
        pass
    next(y_stages)
    s_slot(11)
    for _ in y_stages:
        pass
    s_slot(12)
    r_b.last()
    s_end()
    inv0, inv1 = x_inv
    for _ in y_stages:
        pass
    t10 = left1[0:BS].T
    mine = lt[...].reshape(512, BS).T
    ri = lax.broadcasted_iota(jnp.int32, (BS, 512), 0)
    ci = lax.broadcasted_iota(jnp.int32, (BS, 512), 1)
    unit = jnp.where(ci == ri + me * BS, -1.0, 0.0)
    a = jnp.where(me < 2, unit, mine)
    w1 = mm(a[:, BS:], inv1)
    w0 = mm(a[:, :BS] - mm(w1, t10), inv0)

    def left(d):
        cut = slice(d * BS, (d + 1) * BS)
        base = jnp.where(me < 2, 0.0, s_ref[:, cut])
        o_ref[:, cut] = (
            base - mm(w0, st[d, 0:4].reshape(BS, BS)) - mm(w1, st[d, 4:8].reshape(BS, BS))
        )

    left(0)

    def y_copy(half, dev, k, over):
        part = yb.at[c, pl.ds(half * 128, 128)]
        return pltpu.make_async_remote_copy(
            src_ref=part,
            dst_ref=part,
            send_sem=y_send.at[k],
            recv_sem=y_recv.at[2 * over + half],
            device_id=dev,
            device_id_type=MESH,
        )

    over = [y_copy(h, partner, h, 1) for h in range(2)]
    along = [y_copy(0, at_y(1), 2, 0), y_copy(1, at_y(-1), 3, 0), y_copy(1, at_y(1), 4, 0), y_copy(0, at_y(-1), 5, 0)]

    @pl.when(y == 0)
    def _():
        @pl.when(c == 1)
        def _():
            for e in over:
                e.wait_recv()
            o_ref[:, 0:BS] = o_ref[:, 0:BS] - mm(yb[0], rt[0:4, :, 0].reshape(BS, BS))

        yb[c] = mm(o_ref[:, 0:BS], y_inv[0].T)
        for e in over:
            e.start()
        for e in along:
            e.start()

    for d in (1, 2, 3):
        left(d)

    @pl.when(y == 1)
    def _():
        along[0].wait_recv()
        along[0].start()
        over[0].start()
        along[1].wait_recv()
        over[1].start()

    @pl.when(y == 3)
    def _():
        along[1].wait_recv()
        along[1].start()
        over[1].start()
        along[0].wait_recv()
        over[0].start()

    @pl.when(y == 2)
    def _():
        along[0].wait_recv()
        over[0].start()
        along[1].wait_recv()
        over[1].start()

    @pl.when((y != 0) | (c == 0))
    def _():
        for e in over:
            e.wait_recv()

    def right(d):
        cut = slice(d * BS, (d + 1) * BS)
        o_ref[:, cut] = (
            o_ref[:, cut] - mm(yb[0], rt[0:4, :, d].reshape(BS, BS)) - mm(yb[1], rt[4:8, :, d].reshape(BS, BS))
        )

    for d in (1, 2, 3):
        right(d)
        o_out[2 * d].start()
        o_out[2 * d + 1].start()

    @pl.when(y == 0)
    def _():
        o_ref[:, 0:BS] = yb[c]

    @pl.when(y != 0)
    def _():
        right(0)

    o_out[0].start()
    o_out[1].start()

    for e in events:
        e.wait_send()
    for e in over:
        e.wait_send()

    @pl.when((y == 0) | (y == 1))
    def _():
        along[0].wait_send()

    @pl.when((y == 0) | (y == 3))
    def _():
        along[1].wait_send()

    @pl.when(y == 0)
    def _():
        along[2].wait_send()
        along[3].wait_send()

    s_sent()
    t_sent()
    shares_sent()
    for e in o_out:
        e.wait()


N_EVENTS = 80


def shards(cross_cov, left_factor, right_factor):
    f32 = jnp.float32
    out = pl.pallas_call(
        kernel,
        out_shape=jax.ShapeDtypeStruct((BS, 8, 128), f32),
        in_specs=[
            pl.BlockSpec(memory_space=pl.ANY),
            pl.BlockSpec(memory_space=pltpu.VMEM),
            pl.BlockSpec(memory_space=pltpu.VMEM),
        ],
        out_specs=pl.BlockSpec(memory_space=pl.ANY),
        scratch_shapes=[
            pltpu.VMEM((BS, 1024), f32),
            pltpu.VMEM((BS, 1024), f32),
            pltpu.VMEM((NZ, NX, 4, 16, BS), f32),
            pltpu.VMEM((4, 8, 64, BS), f32),
            pltpu.VMEM((8, 2, 64, BS), f32),
            pltpu.VMEM((8, 64, 256), f32),
            pltpu.VMEM((2, BS, BS), f32),
            pltpu.SemaphoreType.DMA((16,)),
            pltpu.SemaphoreType.DMA((N_EVENTS,)),
            pltpu.SemaphoreType.DMA((N_EVENTS,)),
            pltpu.SemaphoreType.DMA((16,)),
            pltpu.SemaphoreType.DMA((5, 8)),
            pltpu.SemaphoreType.DMA((4, 8)),
            pltpu.SemaphoreType.DMA((17,)),
            pltpu.SemaphoreType.DMA((13,)),
            pltpu.SemaphoreType.DMA((6,)),
            pltpu.SemaphoreType.DMA((4,)),
        ],
        compiler_params=pltpu.CompilerParams(collective_id=0, has_side_effects=True, vmem_limit_bytes=60 * 1024 * 1024),
    )(
        cross_cov.reshape(BS, 8, 128),
        left_factor.reshape(BS, 64).T,
        jnp.swapaxes(right_factor.reshape(4, BS, 16), 1, 2),
    )
    return out.reshape(cross_cov.shape)


def solution(mesh):
    return jax.shard_map(
        shards,
        mesh=mesh,
        in_specs=(
            P(None, "prow", None, None, "pcol", None),
            P(None, "prow", None, "pcol"),
            P(None, "pcol", None, "prow"),
        ),
        out_specs=P(None, "prow", None, None, "pcol", None),
        check_vma=False,
    )
```

```python
import functools

import jax
import jax.numpy as jnp
from jax import lax
from jax.experimental import pallas as pl
from jax.experimental.pallas import tpu as pltpu
from jax.sharding import PartitionSpec as P

BS = 256
NX = 4
NZ = 8
NY = 4
R_CUT = 2
LAG = 2
MESH = pl.DeviceIdType.MESH


def mm(a, b):
    return jnp.dot(a, b, precision=lax.Precision.HIGHEST, preferred_element_type=jnp.float32)


def halves(a):
    high = a.astype(jnp.bfloat16)
    return high, (a - high.astype(jnp.float32)).astype(jnp.bfloat16)


def mm3(a, b):
    (ah, al), (bh, bl) = a, b

    def dot(p, q):
        return jnp.dot(p, q, preferred_element_type=jnp.float32)

    return dot(ah, bh) + (dot(ah, bl) + dot(al, bh))


def inverse_stages(ts, result):
    n, b = ts[0].shape[0], 32
    m = n // b
    rows = lax.broadcasted_iota(jnp.int32, (n, n), 0)
    cols = lax.broadcasted_iota(jnp.int32, (n, n), 1)
    same = (rows >> 5) == (cols >> 5)
    wide = (
        (lax.broadcasted_iota(jnp.int32, (b, n), 1) & (b - 1)) == lax.broadcasted_iota(jnp.int32, (b, n), 0)
    ).astype(jnp.float32)
    tall = (
        (lax.broadcasted_iota(jnp.int32, (n, b), 0) & (b - 1)) == lax.broadcasted_iota(jnp.int32, (n, b), 1)
    ).astype(jnp.float32)
    ts = [jnp.where(rows >= cols, t, 0.0) for t in ts]
    blocks = jnp.concatenate([mm(jnp.where(same, t, 0.0), tall).reshape(m, b, b) for t in ts], axis=0)
    bi = lax.broadcasted_iota(jnp.int32, blocks.shape, 1)
    bj = lax.broadcasted_iota(jnp.int32, blocks.shape, 2)
    diag = jnp.sum(jnp.where(bi == bj, blocks, 0.0), axis=2, keepdims=True)
    rdiag = 1.0 / diag
    lower = jnp.where(bi > bj, blocks * rdiag, 0.0)
    inv = jnp.where(bi == bj, rdiag, 0.0)
    yield
    for j in range(b - 1):
        inv = inv - lower[:, :, j : j + 1] * inv[:, j : j + 1, :]
        if j == b // 2:
            yield
    fulls = [jnp.where(same, mm(inv[k * m : k * m + m].reshape(n, b), wide), 0.0) for k in range(len(ts))]
    yield
    for shift in (5, 6, 7):
        off = ((rows >> (shift + 1)) == (cols >> (shift + 1))) & ((rows >> shift) != (cols >> shift))
        parts = [mm(full, jnp.where(off, t, 0.0)) for full, t in zip(fulls, ts)]
        fulls = [full - mm(part, full) for full, part in zip(fulls, parts)]
        yield
    result.extend(fulls)


def kernel(s_hbm, l_ref, r_ref, o_hbm, s_ref, o_ref, rt, st, tx, lt, yb, xv, rh, rl, io_sem, send_sem, recv_sem, sh_send, s_send, s_recv, t_send, t_recv, y_send, y_recv):
    me = lax.axis_index("prow")
    col = lax.axis_index("pcol")
    z, x = me // NX, me % NX
    y, c = col // 2, col % 2

    def at_x(k):
        return (z * NX + (x + k + NX) % NX, col)

    def at_z(k):
        return (((z + k + NZ) % NZ) * NX + x, col)

    def at_y(k):
        return (me, ((y + k + NY) % NY) * 2 + c)

    partner = (me, y * 2 + 1 - c)

    s_in = [
        pltpu.make_async_copy(s_hbm.at[:, h, :], s_ref.at[:, h * 128 : (h + 1) * 128], io_sem.at[h]) for h in range(8)
    ]

    def write(d, value):
        for h in range(2):
            o_hbm[pl.ds(2 * d + h, BS, stride=8), :] = value[:, h * 128 : (h + 1) * 128]

    s_in.append(pltpu.make_async_copy(l_ref, lt.at[col], io_sem.at[16]))
    s_in.append(pltpu.make_async_copy(r_ref, rt.at[z, x], io_sem.at[17]))
    for e in s_in:
        e.start()
    barrier = pltpu.get_barrier_semaphore()
    near = [at_x(1), at_x(-1), at_x(2), at_z(1), at_z(-1), at_y(1), at_y(-1), at_y(2), partner]
    for dev in near:
        pl.semaphore_signal(barrier, inc=1, device_id=dev, device_id_type=MESH)
    pl.semaphore_wait(barrier, len(near))

    for e in s_in:
        e.wait()
    for root in range(2):

        @pl.when(me == root)
        def _():
            st[root, root * 4 : root * 4 + 4] = s_ref[:, root * BS : (root + 1) * BS].reshape(4, 64, BS)
            tx[col, root, root * 16 : root * 16 + 16] = lt[col, root * 16 : root * 16 + 16]

    events = []

    def send(src, dst, dev):
        k = len(events)
        copy = pltpu.make_async_remote_copy(
            src_ref=src, dst_ref=dst, send_sem=send_sem.at[k], recv_sem=recv_sem.at[k], device_id=dev, device_id_type=MESH
        )
        copy.start()
        events.append(copy)
        return copy

    def same(ref, dev):
        return send(ref, ref, dev)

    def remote(src, dst, ssem, rsem, dev):
        return pltpu.make_async_remote_copy(
            src_ref=src, dst_ref=dst, send_sem=ssem, recv_sem=rsem, device_id=dev, device_id_type=MESH
        )

    dist = jnp.where(z <= NZ // 2, z, NZ - z)
    zdir = jnp.where(z <= NZ // 2, 1, -1)
    passes_on = ((z >= 1) & (z <= 3)) | (z >= 6)

    def s_share(root, k, d):
        return remote(
            s_ref.at[pl.ds(k * 64, 64), pl.ds(d * BS, BS)],
            st.at[d, root * 4 + k],
            sh_send.at[k * 4 + d],
            s_recv.at[0, root * 4 + k],
            (d, col),
        )

    def s_along(k, d, which):
        return remote(st.at[x, k], st.at[x, k], s_send.at[which, k], s_recv.at[0, k], at_z(d))

    def s_across(k, which):
        return remote(st.at[x, k], st.at[x, k], s_send.at[2 + which, k], s_recv.at[1 + which, k], at_x(1 - 2 * which))

    def s_over(k):
        d = 1 - 2 * (k % 2)
        part = st.at[(x - d + NX) % NX, k]
        return remote(part, part, s_send.at[4, k], s_recv.at[3, k], at_x(d))

    def feeds(k):
        return z == 1 + (NZ - 2) * ((k // 2 + k) % 2)

    def s_back(k):
        part = st.at[(x + 2) % NX, k]
        return remote(part, part, s_send.at[5, k], s_recv.at[3, k], (x, col))

    def s_slot(j):
        turn = j - dist

        @pl.when((turn >= 0) & (turn < 8))
        def _():
            k = turn // 2 + 4 * (turn % 2)

            @pl.when((z != 0) | (x != k // 4))
            def _():
                s_along(k, 1, 0).wait_recv()

            @pl.when(z == 0)
            def _():
                s_along(k, 1, 0).start()
                s_along(k, -1, 1).start()

            @pl.when(passes_on)
            def _():
                s_along(k, zdir, 0).start()

            @pl.when(z != 0)
            def _():
                s_across(k, 0).start()
                s_across(k, 1).start()

        if LAG <= j < LAG + 8:

            @pl.when(z == 0)
            def _():
                k = (j - LAG) // 2 + 4 * ((j - LAG) % 2)
                s_across(k, 0).start()
                s_across(k, 1).start()

        @pl.when((turn >= 1) & (turn < 9) & (z != 0))
        def _():
            k = (turn - 1) // 2 + 4 * ((turn - 1) % 2)
            s_across(k, 0).wait_recv()
            s_across(k, 1).wait_recv()
            s_over(k).start()

        @pl.when((turn >= 2) & (turn < 10) & (dist == 1))
        def _():
            k = (turn - 2) // 2 + 4 * ((turn - 2) % 2)

            @pl.when(feeds(k))
            def _():
                s_over(k).wait_recv()
                s_back(k).start()

    def s_end():
        @pl.when(z == 0)
        def _():
            for k in range(8):
                s_across(k, 0).wait_recv()
                s_across(k, 1).wait_recv()

        for k in range(8):

            @pl.when(jnp.logical_not(feeds(k)))
            def _():
                s_over(k).wait_recv()

    def s_sent():
        @pl.when((z == 0) | passes_on)
        def _():
            for k in range(8):
                s_along(k, 1, 0).wait_send()

        @pl.when(z == 0)
        def _():
            for k in range(8):
                s_along(k, -1, 1).wait_send()

        for k in range(8):
            s_across(k, 0).wait_send()
            s_across(k, 1).wait_send()

            @pl.when(z != 0)
            def _():
                s_over(k).wait_send()

            @pl.when(feeds(k))
            def _():
                s_back(k).wait_send()

    def t_share(root, d):
        return remote(
            lt.at[col, pl.ds(d * 16, 16)],
            tx.at[col, root, pl.ds(d * 16, 16)],
            t_send.at[d],
            t_recv.at[root],
            (d, col),
        )

    quarter = tx.at[col, :, pl.ds(x * 16, 16)]
    t_along = [remote(quarter, quarter, t_send.at[4 + w], t_recv.at[2], at_z(d)) for w, d in enumerate((1, -1, zdir))]
    t_across = [remote(quarter, quarter, t_send.at[7 + w], t_recv.at[3 + w], at_x(d)) for w, d in enumerate((1, -1, 2))]
    t_up = [remote(tx.at[col], tx.at[col], t_send.at[10 + w], t_recv.at[6 + w], at_y(d)) for w, d in enumerate((1, -1, 2))]

    def t_over(w):
        part = tx.at[((y - (0, 1, -1, 2)[w] + NY) % NY) * 2 + c]
        return remote(part, part, t_send.at[13 + w], t_recv.at[9 + w], partner)

    def t_slot(n):
        @pl.when(dist == n)
        def _():
            if n == 0:
                for root in range(2):

                    @pl.when(x != root)
                    def _():
                        t_share(root, x).wait_recv()

                t_along[0].start()
                t_along[1].start()
            else:
                t_along[2].wait_recv()

                @pl.when(passes_on)
                def _():
                    t_along[2].start()

            for e in t_across:
                e.start()

        @pl.when(dist == n - 1)
        def _():
            for e in t_across:
                e.wait_recv()
            for e in t_up:
                e.start()
            t_over(0).start()

    def t_step():
        for w in range(3):
            t_up[w].wait_recv()
            t_over(w + 1).start()

    def t_end():
        for w in range(4):
            t_over(w).wait_recv()

    def t_sent():
        @pl.when(z == 0)
        def _():
            t_along[0].wait_send()
            t_along[1].wait_send()

        @pl.when(passes_on)
        def _():
            t_along[2].wait_send()

        for e in t_across + t_up + [t_over(w) for w in range(4)]:
            e.wait_send()

    def t_shares():
        for root in range(2):

            @pl.when(me == root)
            def _():
                for d in range(NX):
                    if d != root:
                        t_share(root, d).start()

    def s_shares(k):
        for root in range(2):

            @pl.when(me == root)
            def _():
                for d in range(NX):
                    if d != root:
                        s_share(root, k, d).start()

    def shares_sent():
        for root in range(2):

            @pl.when(me == root)
            def _():
                for d in range(NX):
                    if d != root:
                        t_share(root, d).wait_send()
                        for k in range(4):
                            s_share(root, k, d).wait_send()

    class Across:
        def __init__(self, view, plus, minus):
            self.view, self.most = view, {1: plus, -1: minus}
            self.sent = {}

        def on(self, d, s, off):
            src = (z - d * (s - 1) + NZ) % NZ
            self.sent[d, s, off] = same(self.view(src, (x + off + NX) % NX), at_z(d))

        def first(self):
            self.xs = [same(self.view(z, x), at_x(k)) for k in (1, -1, 2)]
            for d in (1, -1):
                self.on(d, 1, 0)

        def step(self, s):
            if s == 1:
                for e, k in zip(self.xs, (1, -1, 2)):
                    e.wait_recv()
                    for d in (1, -1):
                        self.on(d, 1, -k)
                return
            for off in (0, -1, 1, -2):
                for d in (1, -1):
                    if (d, s - 1, off) in self.sent:
                        self.sent[d, s - 1, off].wait_recv()
                    if s <= self.most[d]:
                        self.on(d, s, off)

    class Along:
        def __init__(self, view, plus, minus):
            self.view, self.most = view, {1: plus, -1: minus}
            self.zs, self.xs, self.fs = {}, {}, []

        def to_x(self, key, src, d):
            self.xs[key] = (src, d, {k: same(self.view(src, x), at_x(k)) for k in (1, -1)})

        def first(self):
            for d in (1, -1):
                self.zs[d, 1] = same(self.view(z, x), at_z(d))
            self.to_x((1, 1), z, 1 if self.most[1] == 4 else -1)

        def step(self, s):
            for d in (1, -1):
                if s > 1 and (d, s - 1) in self.zs:
                    self.zs[d, s - 1].wait_recv()
                    src = (z - d * (s - 1) + NZ) % NZ
                    if s <= self.most[d]:
                        self.zs[d, s] = same(self.view(src, x), at_z(d))
                    self.to_x((d, s), src, d if s < 5 else -d)

        def cross(self, s):
            for d in (1, -1):
                if (d, s) in self.xs:
                    self.forward((d, s))

        def forward(self, key):
            src, d, sent = self.xs[key]
            sent[1].wait_recv()
            sent[-1].wait_recv()
            self.fs.append(same(self.view(src, (x - d + NX) % NX), at_x(d)))

        def last(self):
            for e in self.fs:
                e.wait_recv()

    def blocks(first, number):
        def view(zz, xx):
            return rt.at[zz, xx, first : first + number]

        return view

    r_a = Across(blocks(0, R_CUT), 4, 3)
    r_b = Along(blocks(R_CUT, 4 - R_CUT), 4, 3)

    class Panel:
        def __init__(self, ref):
            self.ref = ref

        def first(self):
            self.es = [same(self.ref.at[col], at_y(k)) for k in (1, -1, 2)]
            self.ps = [same(self.ref.at[col], partner)]

        def step(self):
            for k, e in zip((1, -1, 2), self.es):
                e.wait_recv()
                self.ps.append(same(self.ref.at[((y - k + NY) % NY) * 2 + c], partner))

        def last(self):
            for e in self.ps:
                e.wait_recv()

    l_p = Panel(lt)

    def panel_of(root):
        return tx[:, root].reshape(512, BS)

    t_shares()
    r_a.first()
    r_b.first()
    l_p.first()
    t_slot(0)
    for k in range(4):
        s_shares(k)
    r_a.step(1)
    r_b.step(2)
    t_slot(1)
    s_slot(0)
    r_b.step(3)
    r_a.step(2)
    t_slot(2)
    s_slot(1)
    r_b.cross(1)
    r_b.step(4)
    t_slot(3)
    s_slot(2)
    r_a.step(3)
    r_b.cross(2)
    t_slot(4)
    s_slot(3)
    r_b.step(5)
    t_slot(5)
    s_slot(4)
    r_b.cross(3)
    r_a.step(4)
    l_p.step()
    s_slot(5)
    t_step()
    r_b.cross(4)
    r_b.cross(5)
    l_p.last()
    t_end()
    r_a.step(5)
    pair = []
    stages = inverse_stages(
        [tx[pl.ds(4 * c, 4), c].reshape(BS, BS).T, rt[pl.ds(4 * c, 4), :, 0].reshape(BS, BS).T], pair
    )
    next(stages)
    s_slot(6)
    next(stages)
    s_slot(7)
    next(stages)
    s_slot(8)
    next(stages)
    s_slot(9)
    next(stages)
    s_slot(10)
    for _ in stages:
        pass
    xv[c] = pair[0]
    xv_copy = same(xv.at[c], partner)
    s_slot(11)
    s_slot(12)
    r_b.last()
    left1 = panel_of(1)
    xv_copy.wait_recv()
    inv0, inv1 = xv[0], xv[1]
    t10 = left1[0:BS].T
    mine = lt[...].reshape(512, BS).T
    ri = lax.broadcasted_iota(jnp.int32, (BS, 512), 0)
    ci = lax.broadcasted_iota(jnp.int32, (BS, 512), 1)
    unit = jnp.where(ci == ri + me * BS, -1.0, 0.0)
    a = jnp.where(me < 2, unit, mine)
    w1 = mm(a[:, BS:], inv1)
    w0 = mm(a[:, :BS] - mm(w1, t10), inv0)

    wide = halves(jnp.concatenate([w0, w1], axis=1))

    def left(d):
        cut = slice(d * BS, (d + 1) * BS)
        base = jnp.where(me < 2, 0.0, s_ref[:, cut])
        o_ref[:, cut] = base - mm3(wide, halves(st[d].reshape(2 * BS, BS)))

    s_end()
    left(0)

    def y_copy(half, dev, k, over):
        part = yb.at[c, pl.ds(half * 128, 128)]
        return pltpu.make_async_remote_copy(
            src_ref=part,
            dst_ref=part,
            send_sem=y_send.at[k],
            recv_sem=y_recv.at[2 * over + half],
            device_id=dev,
            device_id_type=MESH,
        )

    over = [y_copy(h, partner, h, 1) for h in range(2)]
    along = [y_copy(0, at_y(1), 2, 0), y_copy(1, at_y(-1), 3, 0), y_copy(1, at_y(1), 4, 0), y_copy(0, at_y(-1), 5, 0)]

    @pl.when(y == 0)
    def _():
        @pl.when(c == 1)
        def _():
            for e in over:
                e.wait_recv()
            o_ref[:, 0:BS] = o_ref[:, 0:BS] - mm(yb[0], rt[0:4, :, 0].reshape(BS, BS))

        yb[c] = mm(o_ref[:, 0:BS], pair[1].T)
        for e in over:
            e.start()
        for e in along:
            e.start()

    for d in (1, 2, 3):
        left(d)
    for d in range(4):
        high, low = halves(rt[:, :, d].reshape(2 * BS, BS))
        rh[d] = high
        rl[d] = low
    for e in events:
        e.wait_send()
    s_sent()
    t_sent()
    shares_sent()

    @pl.when(y == 1)
    def _():
        along[0].wait_recv()
        along[0].start()
        over[0].start()
        along[1].wait_recv()
        over[1].start()

    @pl.when(y == 3)
    def _():
        along[1].wait_recv()
        along[1].start()
        over[1].start()
        along[0].wait_recv()
        over[0].start()

    @pl.when(y == 2)
    def _():
        along[0].wait_recv()
        over[0].start()
        along[1].wait_recv()
        over[1].start()

    @pl.when((y != 0) | (c == 0))
    def _():
        for e in over:
            e.wait_recv()

    both = halves(jnp.concatenate([yb[0], yb[1]], axis=1))

    def right(d):
        return o_ref[:, d * BS : (d + 1) * BS] - mm3(both, (rh[d], rl[d]))

    for d in (1, 2, 3):
        write(d, right(d))

    @pl.when(y == 0)
    def _():
        write(0, yb[c])

    @pl.when(y != 0)
    def _():
        write(0, right(0))

    for e in over:
        e.wait_send()

    @pl.when((y == 0) | (y == 1))
    def _():
        along[0].wait_send()

    @pl.when((y == 0) | (y == 3))
    def _():
        along[1].wait_send()

    @pl.when(y == 0)
    def _():
        along[2].wait_send()
        along[3].wait_send()


N_EVENTS = 80


def shards(cross_cov, left_factor, right_factor):
    f32 = jnp.float32
    out = pl.pallas_call(
        kernel,
        out_shape=jax.ShapeDtypeStruct((BS * 8, 128), f32),
        in_specs=[
            pl.BlockSpec(memory_space=pltpu.HBM),
            pl.BlockSpec(memory_space=pltpu.HBM),
            pl.BlockSpec(memory_space=pltpu.HBM),
        ],
        out_specs=pl.BlockSpec(memory_space=pltpu.VMEM),
        scratch_shapes=[
            pltpu.VMEM((BS, 1024), f32),
            pltpu.VMEM((BS, 1024), f32),
            pltpu.VMEM((NZ, NX, 4, 16, BS), f32),
            pltpu.VMEM((4, 8, 64, BS), f32),
            pltpu.VMEM((8, 2, 64, BS), f32),
            pltpu.VMEM((8, 64, 256), f32),
            pltpu.VMEM((2, BS, BS), f32),
            pltpu.VMEM((2, BS, BS), f32),
            pltpu.VMEM((4, 2 * BS, BS), jnp.bfloat16),
            pltpu.VMEM((4, 2 * BS, BS), jnp.bfloat16),
            pltpu.SemaphoreType.DMA((18,)),
            pltpu.SemaphoreType.DMA((N_EVENTS,)),
            pltpu.SemaphoreType.DMA((N_EVENTS,)),
            pltpu.SemaphoreType.DMA((16,)),
            pltpu.SemaphoreType.DMA((6, 8)),
            pltpu.SemaphoreType.DMA((4, 8)),
            pltpu.SemaphoreType.DMA((17,)),
            pltpu.SemaphoreType.DMA((13,)),
            pltpu.SemaphoreType.DMA((6,)),
            pltpu.SemaphoreType.DMA((4,)),
        ],
        compiler_params=pltpu.CompilerParams(collective_id=0, has_side_effects=True, vmem_limit_bytes=55000000),
    )(
        cross_cov.reshape(BS, 8, 128),
        left_factor.reshape(BS, 64).T,
        jnp.swapaxes(right_factor.reshape(4, BS, 16), 1, 2),
    )
    return out.reshape(cross_cov.shape)


def solution(mesh):
    return jax.shard_map(
        shards,
        mesh=mesh,
        in_specs=(
            P(None, "prow", None, None, "pcol", None),
            P(None, "prow", None, "pcol"),
            P(None, "pcol", None, "prow"),
        ),
        out_specs=P(None, "prow", None, None, "pcol", None),
        check_vma=False,
    )
```

```python
import functools

import jax
import jax.numpy as jnp
from jax import lax
from jax.experimental import pallas as pl
from jax.experimental.pallas import tpu as pltpu
from jax.sharding import PartitionSpec as P

BS = 256
NX = 4
NZ = 8
NY = 4
R_CUT = 2
LAG = 2
MESH = pl.DeviceIdType.MESH


def mm(a, b):
    return jnp.dot(a, b, precision=lax.Precision.HIGHEST, preferred_element_type=jnp.float32)


def halves(a):
    high = a.astype(jnp.bfloat16)
    return high, (a - high.astype(jnp.float32)).astype(jnp.bfloat16)


def mm3(a, b):
    (ah, al), (bh, bl) = a, b

    def dot(p, q):
        return jnp.dot(p, q, preferred_element_type=jnp.float32)

    return dot(ah, bh) + (dot(ah, bl) + dot(al, bh))


def inverse_stages(ts, result):
    n, b = ts[0].shape[0], 32
    m = n // b
    rows = lax.broadcasted_iota(jnp.int32, (n, n), 0)
    cols = lax.broadcasted_iota(jnp.int32, (n, n), 1)
    same = (rows >> 5) == (cols >> 5)
    wide = (
        (lax.broadcasted_iota(jnp.int32, (b, n), 1) & (b - 1)) == lax.broadcasted_iota(jnp.int32, (b, n), 0)
    ).astype(jnp.float32)
    tall = (
        (lax.broadcasted_iota(jnp.int32, (n, b), 0) & (b - 1)) == lax.broadcasted_iota(jnp.int32, (n, b), 1)
    ).astype(jnp.float32)
    ts = [jnp.where(rows >= cols, t, 0.0) for t in ts]
    blocks = jnp.concatenate([mm(jnp.where(same, t, 0.0), tall).reshape(m, b, b) for t in ts], axis=0)
    bi = lax.broadcasted_iota(jnp.int32, blocks.shape, 1)
    bj = lax.broadcasted_iota(jnp.int32, blocks.shape, 2)
    diag = jnp.sum(jnp.where(bi == bj, blocks, 0.0), axis=2, keepdims=True)
    rdiag = 1.0 / diag
    lower = jnp.where(bi > bj, blocks * rdiag, 0.0)
    inv = jnp.where(bi == bj, rdiag, 0.0)
    yield
    for j in range(b - 1):
        inv = inv - lower[:, :, j : j + 1] * inv[:, j : j + 1, :]
        if j == b // 2:
            yield
    fulls = [jnp.where(same, mm(inv[k * m : k * m + m].reshape(n, b), wide), 0.0) for k in range(len(ts))]
    yield
    for shift in (5, 6, 7):
        off = ((rows >> (shift + 1)) == (cols >> (shift + 1))) & ((rows >> shift) != (cols >> shift))
        parts = [mm(full, jnp.where(off, t, 0.0)) for full, t in zip(fulls, ts)]
        fulls = [full - mm(part, full) for full, part in zip(fulls, parts)]
        yield
    result.extend(fulls)


def kernel(s_hbm, l_ref, r_ref, o_hbm, s_ref, o_ref, rt, st, tx, lt, yb, xv, rh, rl, io_sem, send_sem, recv_sem, sh_send, s_send, s_recv, t_send, t_recv, y_send, y_recv):
    me = lax.axis_index("prow")
    col = lax.axis_index("pcol")
    z, x = me // NX, me % NX
    y, c = col // 2, col % 2

    def at_x(k):
        return (z * NX + (x + k + NX) % NX, col)

    def at_z(k):
        return (((z + k + NZ) % NZ) * NX + x, col)

    def at_y(k):
        return (me, ((y + k + NY) % NY) * 2 + c)

    partner = (me, y * 2 + 1 - c)

    s_in = [
        pltpu.make_async_copy(s_hbm.at[:, h, :], s_ref.at[:, h * 128 : (h + 1) * 128], io_sem.at[0]) for h in range(8)
    ]

    def write(d, value):
        for h in range(2):
            o_hbm[pl.ds(2 * d + h, BS, stride=8), :] = value[:, h * 128 : (h + 1) * 128]

    s_in.append(pltpu.make_async_copy(l_ref, lt.at[col], io_sem.at[1]))
    s_in.append(pltpu.make_async_copy(r_ref, rt.at[z, x], io_sem.at[2]))
    for e in s_in:
        e.start()
    barrier = pltpu.get_barrier_semaphore()
    near = [at_x(1), at_x(-1), at_x(2), at_z(1), at_z(-1), at_y(1), at_y(-1), at_y(2), partner]
    for dev in near:
        pl.semaphore_signal(barrier, inc=1, device_id=dev, device_id_type=MESH)
    pl.semaphore_wait(barrier, len(near))

    pltpu.make_async_copy(s_ref, s_ref, io_sem.at[0]).wait()
    s_in[8].wait()
    s_in[9].wait()
    for root in range(2):

        @pl.when(me == root)
        def _():
            st[root, root * 4 : root * 4 + 4] = s_ref[:, root * BS : (root + 1) * BS].reshape(4, 64, BS)
            tx[col, root, root * 16 : root * 16 + 16] = lt[col, root * 16 : root * 16 + 16]

    events = []

    def same(ref, dev, group):
        copy = pltpu.make_async_remote_copy(
            src_ref=ref,
            dst_ref=ref,
            send_sem=send_sem.at[group],
            recv_sem=recv_sem.at[len(events)],
            device_id=dev,
            device_id_type=MESH,
        )
        copy.start()
        events.append(copy)
        return copy

    def all_sent(sem, ref):
        pltpu.make_async_copy(ref, ref, sem).wait()

    def remote(src, dst, ssem, rsem, dev):
        return pltpu.make_async_remote_copy(
            src_ref=src, dst_ref=dst, send_sem=ssem, recv_sem=rsem, device_id=dev, device_id_type=MESH
        )

    dist = jnp.where(z <= NZ // 2, z, NZ - z)
    zdir = jnp.where(z <= NZ // 2, 1, -1)
    passes_on = ((z >= 1) & (z <= 3)) | (z >= 6)

    def s_share(root, k, d):
        return remote(
            s_ref.at[pl.ds(k * 64, 64), pl.ds(d * BS, BS)],
            st.at[d, root * 4 + k],
            sh_send.at[0],
            s_recv.at[0, root * 4 + k],
            (d, col),
        )

    def s_along(k, d, which):
        return remote(st.at[x, k], st.at[x, k], s_send.at[which], s_recv.at[0, k], at_z(d))

    def s_across(k, which):
        return remote(st.at[x, k], st.at[x, k], s_send.at[2], s_recv.at[1, k], at_x(1 - 2 * which))

    def s_over(k):
        d = 1 - 2 * (k % 2)
        part = st.at[(x - d + NX) % NX, k]
        return remote(part, part, s_send.at[3], s_recv.at[2, k], at_x(d))

    def feeds(k):
        return z == 1 + (NZ - 2) * ((k // 2 + k) % 2)

    def s_back(k):
        part = st.at[(x + 2) % NX, k]
        return remote(part, part, s_send.at[4], s_recv.at[2, k], (x, col))

    def s_slot(j):
        turn = j - dist

        @pl.when((turn >= 0) & (turn < 8))
        def _():
            k = turn // 2 + 4 * (turn % 2)

            @pl.when((z != 0) | (x != k // 4))
            def _():
                s_along(k, 1, 0).wait_recv()

            @pl.when(z == 0)
            def _():
                s_along(k, 1, 0).start()
                s_along(k, -1, 1).start()

            @pl.when(passes_on)
            def _():
                s_along(k, zdir, 0).start()

            @pl.when(z != 0)
            def _():
                s_across(k, 0).start()
                s_across(k, 1).start()

        if LAG <= j < LAG + 8:

            @pl.when(z == 0)
            def _():
                k = (j - LAG) // 2 + 4 * ((j - LAG) % 2)
                s_across(k, 0).start()
                s_across(k, 1).start()

        @pl.when((turn >= 1) & (turn < 9) & (z != 0))
        def _():
            k = (turn - 1) // 2 + 4 * ((turn - 1) % 2)
            all_sent(s_recv.at[1, k], st.at[0, 0:2])
            s_over(k).start()

        @pl.when((turn >= 2) & (turn < 10) & (dist == 1))
        def _():
            k = (turn - 2) // 2 + 4 * ((turn - 2) % 2)

            @pl.when(feeds(k))
            def _():
                s_over(k).wait_recv()
                s_back(k).start()

    def s_end():
        @pl.when(z == 0)
        def _():
            for k in range(8):
                all_sent(s_recv.at[1, k], st.at[0, 0:2])

        for k in range(8):

            @pl.when(jnp.logical_not(feeds(k)))
            def _():
                s_over(k).wait_recv()

    def s_sent():
        @pl.when((z == 0) | passes_on)
        def _():
            all_sent(s_send.at[0], st.at[0])

        @pl.when(z == 0)
        def _():
            all_sent(s_send.at[1], st.at[0])

        all_sent(s_send.at[2], st.at[0:2])

        @pl.when(z != 0)
        def _():
            all_sent(s_send.at[3], st.at[0])

        @pl.when(dist == 1)
        def _():
            all_sent(s_send.at[4], st.at[0, 0:4])

    def t_share(root, d):
        return remote(
            lt.at[col, pl.ds(d * 16, 16)],
            tx.at[col, root, pl.ds(d * 16, 16)],
            t_send.at[0],
            t_recv.at[root],
            (d, col),
        )

    quarter = tx.at[col, :, pl.ds(x * 16, 16)]
    t_along = [remote(quarter, quarter, t_send.at[1], t_recv.at[2], at_z(d)) for d in (1, -1, zdir)]
    t_across = [remote(quarter, quarter, t_send.at[2], t_recv.at[3 + w], at_x(d)) for w, d in enumerate((1, -1, 2))]
    t_up = [remote(tx.at[col], tx.at[col], t_send.at[3], t_recv.at[6 + w], at_y(d)) for w, d in enumerate((1, -1, 2))]

    def t_over(w):
        part = tx.at[((y - (0, 1, -1, 2)[w] + NY) % NY) * 2 + c]
        return remote(part, part, t_send.at[4], t_recv.at[9 + w], partner)

    def t_slot(n):
        @pl.when(dist == n)
        def _():
            if n == 0:
                for root in range(2):

                    @pl.when(x != root)
                    def _():
                        t_share(root, x).wait_recv()

                t_along[0].start()
                t_along[1].start()
            else:
                t_along[2].wait_recv()

                @pl.when(passes_on)
                def _():
                    t_along[2].start()

            for e in t_across:
                e.start()

        @pl.when(dist == n - 1)
        def _():
            for e in t_across:
                e.wait_recv()
            for e in t_up:
                e.start()
            t_over(0).start()

    def t_step():
        for w in range(3):
            t_up[w].wait_recv()
            t_over(w + 1).start()

    def t_end():
        for w in range(4):
            t_over(w).wait_recv()

    def t_sent():
        @pl.when(z == 0)
        def _():
            all_sent(t_send.at[1], tx.at[0:2, :, 0:16])

        @pl.when(passes_on)
        def _():
            all_sent(t_send.at[1], tx.at[0, :, 0:16])

        all_sent(t_send.at[2], tx.at[0:3, :, 0:16])
        all_sent(t_send.at[3], tx.at[0:3])
        all_sent(t_send.at[4], tx.at[0:4])

    def t_shares():
        for root in range(2):

            @pl.when(me == root)
            def _():
                for d in range(NX):
                    if d != root:
                        t_share(root, d).start()

    def s_shares(k):
        for root in range(2):

            @pl.when(me == root)
            def _():
                for d in range(NX):
                    if d != root:
                        s_share(root, k, d).start()

    def shares_sent():
        @pl.when(me < 2)
        def _():
            all_sent(t_send.at[0], lt.at[0, 0:48])
            all_sent(sh_send.at[0], st.at[0:3, 0:4])

    class Across:
        def __init__(self, view, plus, minus):
            self.view, self.most = view, {1: plus, -1: minus}
            self.sent = {}

        def on(self, d, s, off):
            src = (z - d * (s - 1) + NZ) % NZ
            self.sent[d, s, off] = same(self.view(src, (x + off + NX) % NX), at_z(d), 0)

        def first(self):
            self.xs = [same(self.view(z, x), at_x(k), 0) for k in (1, -1, 2)]
            for d in (1, -1):
                self.on(d, 1, 0)

        def step(self, s):
            if s == 1:
                for e, k in zip(self.xs, (1, -1, 2)):
                    e.wait_recv()
                    for d in (1, -1):
                        self.on(d, 1, -k)
                return
            for off in (0, -1, 1, -2):
                for d in (1, -1):
                    if (d, s - 1, off) in self.sent:
                        self.sent[d, s - 1, off].wait_recv()
                    if s <= self.most[d]:
                        self.on(d, s, off)

    class Along:
        def __init__(self, view, plus, minus):
            self.view, self.most = view, {1: plus, -1: minus}
            self.zs, self.xs, self.fs = {}, {}, []

        def to_x(self, key, src, d):
            self.xs[key] = (src, d, {k: same(self.view(src, x), at_x(k), 1) for k in (1, -1)})

        def first(self):
            for d in (1, -1):
                self.zs[d, 1] = same(self.view(z, x), at_z(d), 1)
            self.to_x((1, 1), z, 1 if self.most[1] == 4 else -1)

        def step(self, s):
            for d in (1, -1):
                if s > 1 and (d, s - 1) in self.zs:
                    self.zs[d, s - 1].wait_recv()
                    src = (z - d * (s - 1) + NZ) % NZ
                    if s <= self.most[d]:
                        self.zs[d, s] = same(self.view(src, x), at_z(d), 1)
                    self.to_x((d, s), src, d if s < 5 else -d)

        def cross(self, s):
            for d in (1, -1):
                if (d, s) in self.xs:
                    self.forward((d, s))

        def forward(self, key):
            src, d, sent = self.xs[key]
            sent[1].wait_recv()
            sent[-1].wait_recv()
            self.fs.append(same(self.view(src, (x - d + NX) % NX), at_x(d), 1))

        def last(self):
            for e in self.fs:
                e.wait_recv()

    def blocks(first, number):
        def view(zz, xx):
            return rt.at[zz, xx, first : first + number]

        return view

    r_a = Across(blocks(0, R_CUT), 4, 3)
    r_b = Along(blocks(R_CUT, 4 - R_CUT), 4, 3)

    class Panel:
        def __init__(self, ref):
            self.ref = ref

        def first(self):
            self.es = [same(self.ref.at[col], at_y(k), 2) for k in (1, -1, 2)]
            self.ps = [same(self.ref.at[col], partner, 2)]

        def step(self):
            for k, e in zip((1, -1, 2), self.es):
                e.wait_recv()
                self.ps.append(same(self.ref.at[((y - k + NY) % NY) * 2 + c], partner, 2))

        def last(self):
            for e in self.ps:
                e.wait_recv()

    l_p = Panel(lt)

    def panel_of(root):
        return tx[:, root].reshape(512, BS)

    t_shares()
    r_a.first()
    r_b.first()
    l_p.first()
    t_slot(0)
    for k in range(4):
        s_shares(k)
    r_a.step(1)
    r_b.step(2)
    t_slot(1)
    s_slot(0)
    r_b.step(3)
    r_a.step(2)
    t_slot(2)
    s_slot(1)
    r_b.cross(1)
    r_b.step(4)
    t_slot(3)
    s_slot(2)
    r_a.step(3)
    r_b.cross(2)
    t_slot(4)
    s_slot(3)
    r_b.step(5)
    t_slot(5)
    s_slot(4)
    r_b.cross(3)
    r_a.step(4)
    l_p.step()
    s_slot(5)
    t_step()
    r_b.cross(4)
    r_b.cross(5)
    l_p.last()
    t_end()
    r_a.step(5)
    pair = []
    stages = inverse_stages(
        [tx[pl.ds(4 * c, 4), c].reshape(BS, BS).T, rt[pl.ds(4 * c, 4), :, 0].reshape(BS, BS).T], pair
    )
    next(stages)
    s_slot(6)
    next(stages)
    s_slot(7)
    next(stages)
    s_slot(8)
    next(stages)
    s_slot(9)
    next(stages)
    s_slot(10)
    for _ in stages:
        pass
    xv[c] = pair[0]
    xv_copy = same(xv.at[c], partner, 3)
    s_slot(11)
    s_slot(12)
    r_b.last()
    left1 = panel_of(1)
    xv_copy.wait_recv()
    inv0, inv1 = xv[0], xv[1]
    t10 = left1[0:BS].T
    mine = lt[...].reshape(512, BS).T
    ri = lax.broadcasted_iota(jnp.int32, (BS, 512), 0)
    ci = lax.broadcasted_iota(jnp.int32, (BS, 512), 1)
    unit = jnp.where(ci == ri + me * BS, -1.0, 0.0)
    a = jnp.where(me < 2, unit, mine)
    w1 = mm(a[:, BS:], inv1)
    w0 = mm(a[:, :BS] - mm(w1, t10), inv0)

    wide = halves(jnp.concatenate([w0, w1], axis=1))

    def left(d):
        cut = slice(d * BS, (d + 1) * BS)
        base = jnp.where(me < 2, 0.0, s_ref[:, cut])
        o_ref[:, cut] = base - mm3(wide, halves(st[d].reshape(2 * BS, BS)))

    s_end()
    left(0)

    def y_copy(half, dev, k, over):
        part = yb.at[c, pl.ds(half * 128, 128)]
        return pltpu.make_async_remote_copy(
            src_ref=part,
            dst_ref=part,
            send_sem=y_send.at[k],
            recv_sem=y_recv.at[2 * over + half],
            device_id=dev,
            device_id_type=MESH,
        )

    over = [y_copy(h, partner, h, 1) for h in range(2)]
    along = [y_copy(0, at_y(1), 2, 0), y_copy(1, at_y(-1), 3, 0), y_copy(1, at_y(1), 4, 0), y_copy(0, at_y(-1), 5, 0)]

    @pl.when(y == 0)
    def _():
        @pl.when(c == 1)
        def _():
            for e in over:
                e.wait_recv()
            o_ref[:, 0:BS] = o_ref[:, 0:BS] - mm(yb[0], rt[0:4, :, 0].reshape(BS, BS))

        yb[c] = mm(o_ref[:, 0:BS], pair[1].T)
        for e in over:
            e.start()
        for e in along:
            e.start()

    for d in (1, 2, 3):
        left(d)
    for d in range(4):
        high, low = halves(rt[:, :, d].reshape(2 * BS, BS))
        rh[d] = high
        rl[d] = low
    all_sent(send_sem.at[0], s_ref.at[0:248])
    all_sent(send_sem.at[1], s_ref.at[0:248])
    all_sent(send_sem.at[2], lt.at[0:7])
    all_sent(send_sem.at[3], xv.at[0])
    s_sent()
    t_sent()
    shares_sent()

    @pl.when(y == 1)
    def _():
        along[0].wait_recv()
        along[0].start()
        over[0].start()
        along[1].wait_recv()
        over[1].start()

    @pl.when(y == 3)
    def _():
        along[1].wait_recv()
        along[1].start()
        over[1].start()
        along[0].wait_recv()
        over[0].start()

    @pl.when(y == 2)
    def _():
        along[0].wait_recv()
        over[0].start()
        along[1].wait_recv()
        over[1].start()

    @pl.when((y != 0) | (c == 0))
    def _():
        for e in over:
            e.wait_recv()

    both = halves(jnp.concatenate([yb[0], yb[1]], axis=1))

    def right(d):
        return o_ref[:, d * BS : (d + 1) * BS] - mm3(both, (rh[d], rl[d]))

    for d in (1, 2, 3):
        write(d, right(d))

    @pl.when(y == 0)
    def _():
        write(0, yb[c])

    @pl.when(y != 0)
    def _():
        write(0, right(0))

    for e in over:
        e.wait_send()

    @pl.when((y == 0) | (y == 1))
    def _():
        along[0].wait_send()

    @pl.when((y == 0) | (y == 3))
    def _():
        along[1].wait_send()

    @pl.when(y == 0)
    def _():
        along[2].wait_send()
        along[3].wait_send()


N_EVENTS = 70


def shards(cross_cov, left_factor, right_factor):
    f32 = jnp.float32
    out = pl.pallas_call(
        kernel,
        out_shape=jax.ShapeDtypeStruct((BS * 8, 128), f32),
        in_specs=[
            pl.BlockSpec(memory_space=pltpu.HBM),
            pl.BlockSpec(memory_space=pltpu.HBM),
            pl.BlockSpec(memory_space=pltpu.HBM),
        ],
        out_specs=pl.BlockSpec(memory_space=pltpu.VMEM),
        scratch_shapes=[
            pltpu.VMEM((BS, 1024), f32),
            pltpu.VMEM((BS, 1024), f32),
            pltpu.VMEM((NZ, NX, 4, 16, BS), f32),
            pltpu.VMEM((4, 8, 64, BS), f32),
            pltpu.VMEM((8, 2, 64, BS), f32),
            pltpu.VMEM((8, 64, 256), f32),
            pltpu.VMEM((2, BS, BS), f32),
            pltpu.VMEM((2, BS, BS), f32),
            pltpu.VMEM((4, 2 * BS, BS), jnp.bfloat16),
            pltpu.VMEM((4, 2 * BS, BS), jnp.bfloat16),
            pltpu.SemaphoreType.DMA((3,)),
            pltpu.SemaphoreType.DMA((4,)),
            pltpu.SemaphoreType.DMA((N_EVENTS,)),
            pltpu.SemaphoreType.DMA((1,)),
            pltpu.SemaphoreType.DMA((5,)),
            pltpu.SemaphoreType.DMA((3, 8)),
            pltpu.SemaphoreType.DMA((5,)),
            pltpu.SemaphoreType.DMA((13,)),
            pltpu.SemaphoreType.DMA((6,)),
            pltpu.SemaphoreType.DMA((4,)),
        ],
        compiler_params=pltpu.CompilerParams(collective_id=0, has_side_effects=True, vmem_limit_bytes=55000000),
    )(
        cross_cov.reshape(BS, 8, 128),
        left_factor.reshape(BS, 64).T,
        jnp.swapaxes(right_factor.reshape(4, BS, 16), 1, 2),
    )
    return out.reshape(cross_cov.shape)


def solution(mesh):
    return jax.shard_map(
        shards,
        mesh=mesh,
        in_specs=(
            P(None, "prow", None, None, "pcol", None),
            P(None, "prow", None, "pcol"),
            P(None, "pcol", None, "prow"),
        ),
        out_specs=P(None, "prow", None, None, "pcol", None),
        check_vma=False,
    )
```

```python
import functools

import jax
import jax.numpy as jnp
from jax import lax
from jax.experimental import pallas as pl
from jax.experimental.pallas import tpu as pltpu
from jax.sharding import PartitionSpec as P

BS = 256
NX = 4
NZ = 8
NY = 4
R_CUT = 2
LAG = 2
MESH = pl.DeviceIdType.MESH


def mm(a, b):
    return jnp.dot(a, b, precision=lax.Precision.HIGHEST, preferred_element_type=jnp.float32)


def halves(a):
    high = a.astype(jnp.bfloat16)
    return high, (a - high.astype(jnp.float32)).astype(jnp.bfloat16)


def mm3(a, b):
    (ah, al), (bh, bl) = a, b

    def dot(p, q):
        return jnp.dot(p, q, preferred_element_type=jnp.float32)

    return dot(ah, bh) + (dot(ah, bl) + dot(al, bh))


def inverse_stages(ts, result):
    n, b = ts[0].shape[0], 32
    m = n // b
    rows = lax.broadcasted_iota(jnp.int32, (n, n), 0)
    cols = lax.broadcasted_iota(jnp.int32, (n, n), 1)
    same = (rows >> 5) == (cols >> 5)
    wide = (
        (lax.broadcasted_iota(jnp.int32, (b, n), 1) & (b - 1)) == lax.broadcasted_iota(jnp.int32, (b, n), 0)
    ).astype(jnp.float32)
    tall = (
        (lax.broadcasted_iota(jnp.int32, (n, b), 0) & (b - 1)) == lax.broadcasted_iota(jnp.int32, (n, b), 1)
    ).astype(jnp.float32)
    ts = [jnp.where(rows >= cols, t, 0.0) for t in ts]
    blocks = jnp.concatenate([mm(jnp.where(same, t, 0.0), tall).reshape(m, b, b) for t in ts], axis=0)
    bi = lax.broadcasted_iota(jnp.int32, blocks.shape, 1)
    bj = lax.broadcasted_iota(jnp.int32, blocks.shape, 2)
    diag = jnp.sum(jnp.where(bi == bj, blocks, 0.0), axis=2, keepdims=True)
    rdiag = 1.0 / diag
    lower = jnp.where(bi > bj, blocks * rdiag, 0.0)
    inv = jnp.where(bi == bj, rdiag, 0.0)
    yield
    for j in range(b - 1):
        inv = inv - lower[:, :, j : j + 1] * inv[:, j : j + 1, :]
        if j == b // 2:
            yield
    fulls = [jnp.where(same, mm(inv[k * m : k * m + m].reshape(n, b), wide), 0.0) for k in range(len(ts))]
    yield
    for shift in (5, 6, 7):
        off = ((rows >> (shift + 1)) == (cols >> (shift + 1))) & ((rows >> shift) != (cols >> shift))
        parts = [mm(full, jnp.where(off, t, 0.0)) for full, t in zip(fulls, ts)]
        fulls = [full - mm(part, full) for full, part in zip(fulls, parts)]
        yield
    result.extend(fulls)


def kernel(s_hbm, l_ref, r_ref, o_hbm, s_ref, o_ref, rt, st, tx, lt, yb, xv, rh, rl, io_sem, send_sem, recv_sem, sh_send, s_send, s_recv, t_send, t_recv, y_send, y_recv):
    me = lax.axis_index("prow")
    col = lax.axis_index("pcol")
    z, x = me // NX, me % NX
    y, c = col // 2, col % 2

    def at_x(k):
        return (z * NX + (x + k + NX) % NX, col)

    def at_z(k):
        return (((z + k + NZ) % NZ) * NX + x, col)

    def at_y(k):
        return (me, ((y + k + NY) % NY) * 2 + c)

    partner = (me, y * 2 + 1 - c)

    s_in = [
        pltpu.make_async_copy(s_hbm.at[:, h, :], s_ref.at[:, h * 128 : (h + 1) * 128], io_sem.at[0]) for h in range(8)
    ]

    def write(d, value):
        for h in range(2):
            o_hbm[pl.ds(2 * d + h, BS, stride=8), :] = value[:, h * 128 : (h + 1) * 128]

    s_in.append(pltpu.make_async_copy(l_ref, lt.at[col], io_sem.at[1]))
    s_in.append(pltpu.make_async_copy(r_ref, rt.at[z, x], io_sem.at[2]))
    for e in s_in:
        e.start()
    barrier = pltpu.get_barrier_semaphore()
    near = [at_x(1), at_x(-1), at_x(2), at_z(1), at_z(-1), at_y(1), at_y(-1), at_y(2), partner]
    for dev in near:
        pl.semaphore_signal(barrier, inc=1, device_id=dev, device_id_type=MESH)
    pl.semaphore_wait(barrier, len(near))

    pltpu.make_async_copy(s_ref, s_ref, io_sem.at[0]).wait()
    s_in[8].wait()
    s_in[9].wait()
    for root in range(2):

        @pl.when(me == root)
        def _():
            st[root, root * 4 : root * 4 + 4] = s_ref[:, root * BS : (root + 1) * BS].reshape(4, 64, BS)
            tx[col, root, root * 16 : root * 16 + 16] = lt[col, root * 16 : root * 16 + 16]

    events = []

    def same(ref, dev, group):
        copy = pltpu.make_async_remote_copy(
            src_ref=ref,
            dst_ref=ref,
            send_sem=send_sem.at[group],
            recv_sem=recv_sem.at[len(events)],
            device_id=dev,
            device_id_type=MESH,
        )
        copy.start()
        events.append(copy)
        return copy

    def all_sent(sem, ref):
        pltpu.make_async_copy(ref, ref, sem).wait()

    def remote(src, dst, ssem, rsem, dev):
        return pltpu.make_async_remote_copy(
            src_ref=src, dst_ref=dst, send_sem=ssem, recv_sem=rsem, device_id=dev, device_id_type=MESH
        )

    dist = jnp.where(z <= NZ // 2, z, NZ - z)
    zdir = jnp.where(z <= NZ // 2, 1, -1)
    passes_on = ((z >= 1) & (z <= 3)) | (z >= 6)

    def s_share(root, k, d):
        return remote(
            s_ref.at[pl.ds(k * 64, 64), pl.ds(d * BS, BS)],
            st.at[d, root * 4 + k],
            sh_send.at[0],
            s_recv.at[0, root * 4 + k],
            (d, col),
        )

    def s_along(k, d, which):
        return remote(st.at[x, k], st.at[x, k], s_send.at[which], s_recv.at[0, k], at_z(d))

    def s_across(k, which):
        return remote(st.at[x, k], st.at[x, k], s_send.at[2], s_recv.at[1, k], at_x(1 - 2 * which))

    def s_over(k):
        d = 1 - 2 * (k % 2)
        part = st.at[(x - d + NX) % NX, k]
        return remote(part, part, s_send.at[3], s_recv.at[2, k], at_x(d))

    def feeds(k):
        return z == 1 + (NZ - 2) * ((k // 2 + k) % 2)

    def s_back(k):
        part = st.at[(x + 2) % NX, k]
        return remote(part, part, s_send.at[4], s_recv.at[2, k], (x, col))

    def s_slot(j):
        turn = j - dist

        @pl.when((turn >= 0) & (turn < 8))
        def _():
            k = turn // 2 + 4 * (turn % 2)

            @pl.when((z != 0) | (x != k // 4))
            def _():
                s_along(k, 1, 0).wait_recv()

            @pl.when(z == 0)
            def _():
                s_along(k, 1, 0).start()
                s_along(k, -1, 1).start()

            @pl.when(passes_on)
            def _():
                s_along(k, zdir, 0).start()

            @pl.when(z != 0)
            def _():
                s_across(k, 0).start()
                s_across(k, 1).start()

        if LAG <= j < LAG + 8:

            @pl.when(z == 0)
            def _():
                k = (j - LAG) // 2 + 4 * ((j - LAG) % 2)
                s_across(k, 0).start()
                s_across(k, 1).start()

        @pl.when((turn >= 2) & (turn < 10) & (z != 0))
        def _():
            k = (turn - 2) // 2 + 4 * ((turn - 2) % 2)
            all_sent(s_recv.at[1, k], st.at[0, 0:2])
            s_over(k).start()

        @pl.when((turn >= 5) & (turn < 13) & (dist == 1))
        def _():
            k = (turn - 5) // 2 + 4 * ((turn - 5) % 2)

            @pl.when(feeds(k))
            def _():
                s_over(k).wait_recv()
                s_back(k).start()

    def s_end():
        @pl.when(z == 0)
        def _():
            for k in range(8):
                all_sent(s_recv.at[1, k], st.at[0, 0:2])

        for k in range(8):

            @pl.when(jnp.logical_not(feeds(k)))
            def _():
                s_over(k).wait_recv()

    def s_sent():
        @pl.when((z == 0) | passes_on)
        def _():
            all_sent(s_send.at[0], st.at[0])

        @pl.when(z == 0)
        def _():
            all_sent(s_send.at[1], st.at[0])

        all_sent(s_send.at[2], st.at[0:2])

        @pl.when(z != 0)
        def _():
            all_sent(s_send.at[3], st.at[0])

        @pl.when(dist == 1)
        def _():
            all_sent(s_send.at[4], st.at[0, 0:4])

    def t_share(root, d):
        return remote(
            lt.at[col, pl.ds(d * 16, 16)],
            tx.at[col, root, pl.ds(d * 16, 16)],
            t_send.at[0],
            t_recv.at[root],
            (d, col),
        )

    quarter = tx.at[col, :, pl.ds(x * 16, 16)]
    t_along = [remote(quarter, quarter, t_send.at[1], t_recv.at[2], at_z(d)) for d in (1, -1, zdir)]
    t_across = [remote(quarter, quarter, t_send.at[2], t_recv.at[3 + w], at_x(d)) for w, d in enumerate((1, -1, 2))]
    t_up = [remote(tx.at[col], tx.at[col], t_send.at[3], t_recv.at[6 + w], at_y(d)) for w, d in enumerate((1, -1, 2))]

    def t_over(w):
        part = tx.at[((y - (0, 1, -1, 2)[w] + NY) % NY) * 2 + c]
        return remote(part, part, t_send.at[4], t_recv.at[9 + w], partner)

    def t_slot(n):
        @pl.when(dist == n)
        def _():
            if n == 0:
                for root in range(2):

                    @pl.when(x != root)
                    def _():
                        t_share(root, x).wait_recv()

                t_along[0].start()
                t_along[1].start()
            else:
                t_along[2].wait_recv()

                @pl.when(passes_on)
                def _():
                    t_along[2].start()

            for e in t_across:
                e.start()

        @pl.when(dist == n - 1)
        def _():
            for e in t_across:
                e.wait_recv()
            for e in t_up:
                e.start()
            t_over(0).start()

    def t_step():
        for w in range(3):
            t_up[w].wait_recv()
            t_over(w + 1).start()

    def t_end():
        for w in range(4):
            t_over(w).wait_recv()

    def t_sent():
        @pl.when(z == 0)
        def _():
            all_sent(t_send.at[1], tx.at[0:2, :, 0:16])

        @pl.when(passes_on)
        def _():
            all_sent(t_send.at[1], tx.at[0, :, 0:16])

        all_sent(t_send.at[2], tx.at[0:3, :, 0:16])
        all_sent(t_send.at[3], tx.at[0:3])
        all_sent(t_send.at[4], tx.at[0:4])

    def t_shares():
        for root in range(2):

            @pl.when(me == root)
            def _():
                for d in range(NX):
                    if d != root:
                        t_share(root, d).start()

    def s_shares(k):
        for root in range(2):

            @pl.when(me == root)
            def _():
                for d in range(NX):
                    if d != root:
                        s_share(root, k, d).start()

    def shares_sent():
        @pl.when(me < 2)
        def _():
            all_sent(t_send.at[0], lt.at[0, 0:48])
            all_sent(sh_send.at[0], st.at[0:3, 0:4])

    class Across:
        def __init__(self, view, plus, minus):
            self.view, self.most = view, {1: plus, -1: minus}
            self.sent = {}

        def on(self, d, s, off):
            src = (z - d * (s - 1) + NZ) % NZ
            self.sent[d, s, off] = same(self.view(src, (x + off + NX) % NX), at_z(d), 0)

        def first(self):
            self.xs = [same(self.view(z, x), at_x(k), 0) for k in (1, -1, 2)]
            for d in (1, -1):
                self.on(d, 1, 0)

        def step(self, s):
            if s == 1:
                for e, k in zip(self.xs, (1, -1, 2)):
                    e.wait_recv()
                    for d in (1, -1):
                        self.on(d, 1, -k)
                return
            for off in (0, -1, 1, -2):
                for d in (1, -1):
                    if (d, s - 1, off) in self.sent:
                        self.sent[d, s - 1, off].wait_recv()
                    if s <= self.most[d]:
                        self.on(d, s, off)

    class Along:
        def __init__(self, view, plus, minus):
            self.view, self.most = view, {1: plus, -1: minus}
            self.zs, self.xs, self.fs = {}, {}, []

        def to_x(self, key, src, d):
            self.xs[key] = (src, d, {k: same(self.view(src, x), at_x(k), 1) for k in (1, -1)})

        def first(self):
            for d in (1, -1):
                self.zs[d, 1] = same(self.view(z, x), at_z(d), 1)
            self.to_x((1, 1), z, 1 if self.most[1] == 4 else -1)

        def step(self, s):
            for d in (1, -1):
                if s > 1 and (d, s - 1) in self.zs:
                    self.zs[d, s - 1].wait_recv()
                    src = (z - d * (s - 1) + NZ) % NZ
                    if s <= self.most[d]:
                        self.zs[d, s] = same(self.view(src, x), at_z(d), 1)
                    self.to_x((d, s), src, d if s < 5 else -d)

        def cross(self, s):
            for d in (1, -1):
                if (d, s) in self.xs:
                    self.forward((d, s))

        def forward(self, key):
            src, d, sent = self.xs[key]
            sent[1].wait_recv()
            sent[-1].wait_recv()
            self.fs.append(same(self.view(src, (x - d + NX) % NX), at_x(d), 1))

        def last(self):
            for e in self.fs:
                e.wait_recv()

    def blocks(first, number):
        def view(zz, xx):
            return rt.at[zz, xx, first : first + number]

        return view

    r_a = Across(blocks(0, R_CUT), 4, 3)
    r_b = Along(blocks(R_CUT, 4 - R_CUT), 4, 3)

    class Panel:
        def __init__(self, ref):
            self.ref = ref

        def first(self):
            self.es = [same(self.ref.at[col], at_y(k), 2) for k in (1, -1, 2)]
            self.ps = [same(self.ref.at[col], partner, 2)]

        def step(self):
            for k, e in zip((1, -1, 2), self.es):
                e.wait_recv()
                self.ps.append(same(self.ref.at[((y - k + NY) % NY) * 2 + c], partner, 2))

        def last(self):
            for e in self.ps:
                e.wait_recv()

    l_p = Panel(lt)

    def panel_of(root):
        return tx[:, root].reshape(512, BS)

    t_shares()
    r_a.first()
    r_b.first()
    l_p.first()
    t_slot(0)
    for k in range(4):
        s_shares(k)
    r_a.step(1)
    r_b.step(2)
    t_slot(1)
    s_slot(0)
    r_b.step(3)
    r_a.step(2)
    t_slot(2)
    s_slot(1)
    r_b.cross(1)
    r_b.step(4)
    t_slot(3)
    s_slot(2)
    r_a.step(3)
    r_b.cross(2)
    t_slot(4)
    s_slot(3)
    r_b.step(5)
    t_slot(5)
    s_slot(4)
    r_b.cross(3)
    r_a.step(4)
    l_p.step()
    s_slot(5)
    t_step()
    r_b.cross(4)
    r_b.cross(5)
    l_p.last()
    t_end()
    r_a.step(5)
    pair = []
    stages = inverse_stages(
        [tx[pl.ds(4 * c, 4), c].reshape(BS, BS).T, rt[pl.ds(4 * c, 4), :, 0].reshape(BS, BS).T], pair
    )
    next(stages)
    s_slot(6)
    next(stages)
    s_slot(7)
    next(stages)
    s_slot(8)
    next(stages)
    s_slot(9)
    next(stages)
    s_slot(10)
    for _ in stages:
        pass
    xv[c] = pair[0]
    xv_copy = same(xv.at[c], partner, 3)
    s_slot(11)
    s_slot(12)
    left1 = panel_of(1)
    t10 = left1[0:BS].T
    mine = lt[...].reshape(512, BS).T
    ri = lax.broadcasted_iota(jnp.int32, (BS, 512), 0)
    ci = lax.broadcasted_iota(jnp.int32, (BS, 512), 1)
    unit = jnp.where(ci == ri + me * BS, -1.0, 0.0)
    a = jnp.where(me < 2, unit, mine)
    xv_copy.wait_recv()
    inv0, inv1 = xv[0], xv[1]
    w1 = mm(a[:, BS:], inv1)
    w0 = mm(a[:, :BS] - mm(w1, t10), inv0)
    wide = halves(jnp.concatenate([w0, w1], axis=1))
    s_slot(13)
    r_b.last()

    def left(d):
        cut = slice(d * BS, (d + 1) * BS)
        base = jnp.where(me < 2, 0.0, s_ref[:, cut])
        o_ref[:, cut] = base - mm3(wide, halves(st[d].reshape(2 * BS, BS)))

    s_end()
    left(0)

    def y_copy(half, dev, k, over):
        part = yb.at[c, pl.ds(half * 128, 128)]
        return pltpu.make_async_remote_copy(
            src_ref=part,
            dst_ref=part,
            send_sem=y_send.at[k],
            recv_sem=y_recv.at[2 * over + half],
            device_id=dev,
            device_id_type=MESH,
        )

    over = [y_copy(h, partner, h, 1) for h in range(2)]
    along = [y_copy(0, at_y(1), 2, 0), y_copy(1, at_y(-1), 3, 0), y_copy(1, at_y(1), 4, 0), y_copy(0, at_y(-1), 5, 0)]

    @pl.when(y == 0)
    def _():
        @pl.when(c == 1)
        def _():
            for e in over:
                e.wait_recv()
            o_ref[:, 0:BS] = o_ref[:, 0:BS] - mm(yb[0], rt[0:4, :, 0].reshape(BS, BS))

        yb[c] = mm(o_ref[:, 0:BS], pair[1].T)
        for e in over:
            e.start()
        for e in along:
            e.start()

    for d in (1, 2, 3):
        left(d)
    for d in range(4):
        high, low = halves(rt[:, :, d].reshape(2 * BS, BS))
        rh[d] = high
        rl[d] = low
    all_sent(send_sem.at[0], s_ref.at[0:248])
    all_sent(send_sem.at[1], s_ref.at[0:248])
    all_sent(send_sem.at[2], lt.at[0:7])
    all_sent(send_sem.at[3], xv.at[0])
    s_sent()
    t_sent()
    shares_sent()

    @pl.when(y == 1)
    def _():
        along[0].wait_recv()
        along[0].start()
        over[0].start()
        along[1].wait_recv()
        over[1].start()

    @pl.when(y == 3)
    def _():
        along[1].wait_recv()
        along[1].start()
        over[1].start()
        along[0].wait_recv()
        over[0].start()

    @pl.when(y == 2)
    def _():
        along[0].wait_recv()
        over[0].start()
        along[1].wait_recv()
        over[1].start()

    @pl.when((y != 0) | (c == 0))
    def _():
        for e in over:
            e.wait_recv()

    both = halves(jnp.concatenate([yb[0], yb[1]], axis=1))

    def right(d):
        return o_ref[:, d * BS : (d + 1) * BS] - mm3(both, (rh[d], rl[d]))

    for d in (1, 2, 3):
        write(d, right(d))

    @pl.when(y == 0)
    def _():
        write(0, yb[c])

    @pl.when(y != 0)
    def _():
        write(0, right(0))

    for e in over:
        e.wait_send()

    @pl.when((y == 0) | (y == 1))
    def _():
        along[0].wait_send()

    @pl.when((y == 0) | (y == 3))
    def _():
        along[1].wait_send()

    @pl.when(y == 0)
    def _():
        along[2].wait_send()
        along[3].wait_send()


N_EVENTS = 70


def shards(cross_cov, left_factor, right_factor):
    f32 = jnp.float32
    out = pl.pallas_call(
        kernel,
        out_shape=jax.ShapeDtypeStruct((BS * 8, 128), f32),
        in_specs=[
            pl.BlockSpec(memory_space=pltpu.HBM),
            pl.BlockSpec(memory_space=pltpu.HBM),
            pl.BlockSpec(memory_space=pltpu.HBM),
        ],
        out_specs=pl.BlockSpec(memory_space=pltpu.VMEM),
        scratch_shapes=[
            pltpu.VMEM((BS, 1024), f32),
            pltpu.VMEM((BS, 1024), f32),
            pltpu.VMEM((NZ, NX, 4, 16, BS), f32),
            pltpu.VMEM((4, 8, 64, BS), f32),
            pltpu.VMEM((8, 2, 64, BS), f32),
            pltpu.VMEM((8, 64, 256), f32),
            pltpu.VMEM((2, BS, BS), f32),
            pltpu.VMEM((2, BS, BS), f32),
            pltpu.VMEM((4, 2 * BS, BS), jnp.bfloat16),
            pltpu.VMEM((4, 2 * BS, BS), jnp.bfloat16),
            pltpu.SemaphoreType.DMA((3,)),
            pltpu.SemaphoreType.DMA((4,)),
            pltpu.SemaphoreType.DMA((N_EVENTS,)),
            pltpu.SemaphoreType.DMA((1,)),
            pltpu.SemaphoreType.DMA((5,)),
            pltpu.SemaphoreType.DMA((3, 8)),
            pltpu.SemaphoreType.DMA((5,)),
            pltpu.SemaphoreType.DMA((13,)),
            pltpu.SemaphoreType.DMA((6,)),
            pltpu.SemaphoreType.DMA((4,)),
        ],
        compiler_params=pltpu.CompilerParams(collective_id=0, has_side_effects=True, vmem_limit_bytes=55000000),
    )(
        cross_cov.reshape(BS, 8, 128),
        left_factor.reshape(BS, 64).T,
        jnp.swapaxes(right_factor.reshape(4, BS, 16), 1, 2),
    )
    return out.reshape(cross_cov.shape)


def solution(mesh):
    return jax.shard_map(
        shards,
        mesh=mesh,
        in_specs=(
            P(None, "prow", None, None, "pcol", None),
            P(None, "prow", None, "pcol"),
            P(None, "pcol", None, "prow"),
        ),
        out_specs=P(None, "prow", None, None, "pcol", None),
        check_vma=False,
    )
```

```python
import functools

import jax
import jax.numpy as jnp
from jax import lax
from jax.experimental import pallas as pl
from jax.experimental.pallas import tpu as pltpu
from jax.sharding import PartitionSpec as P

BS = 256
NX = 4
NZ = 8
NY = 4
R_CUT = 2
LAG = 2
MESH = pl.DeviceIdType.MESH


def mm(a, b):
    return jnp.dot(a, b, precision=lax.Precision.HIGHEST, preferred_element_type=jnp.float32)


def halves(a):
    high = a.astype(jnp.bfloat16)
    return high, (a - high.astype(jnp.float32)).astype(jnp.bfloat16)


def mm3(a, b):
    (ah, al), (bh, bl) = a, b

    def dot(p, q):
        return jnp.dot(p, q, preferred_element_type=jnp.float32)

    return dot(ah, bh) + (dot(ah, bl) + dot(al, bh))


def inverse_stages(ts, result):
    n, b = ts[0].shape[0], 32
    m = n // b
    rows = lax.broadcasted_iota(jnp.int32, (n, n), 0)
    cols = lax.broadcasted_iota(jnp.int32, (n, n), 1)
    same = (rows >> 5) == (cols >> 5)
    wide = (
        (lax.broadcasted_iota(jnp.int32, (b, n), 1) & (b - 1)) == lax.broadcasted_iota(jnp.int32, (b, n), 0)
    ).astype(jnp.float32)
    tall = (
        (lax.broadcasted_iota(jnp.int32, (n, b), 0) & (b - 1)) == lax.broadcasted_iota(jnp.int32, (n, b), 1)
    ).astype(jnp.float32)
    ts = [jnp.where(rows >= cols, t, 0.0) for t in ts]
    blocks = jnp.concatenate([mm(jnp.where(same, t, 0.0), tall).reshape(m, b, b) for t in ts], axis=0)
    bi = lax.broadcasted_iota(jnp.int32, blocks.shape, 1)
    bj = lax.broadcasted_iota(jnp.int32, blocks.shape, 2)
    diag = jnp.sum(jnp.where(bi == bj, blocks, 0.0), axis=2, keepdims=True)
    rdiag = 1.0 / diag
    lower = jnp.where(bi > bj, blocks * rdiag, 0.0)
    inv = jnp.where(bi == bj, rdiag, 0.0)
    yield
    for j in range(b - 1):
        inv = inv - lower[:, :, j : j + 1] * inv[:, j : j + 1, :]
        if j == b // 2:
            yield
    fulls = [jnp.where(same, mm(inv[k * m : k * m + m].reshape(n, b), wide), 0.0) for k in range(len(ts))]
    yield
    for shift in (5, 6, 7):
        off = ((rows >> (shift + 1)) == (cols >> (shift + 1))) & ((rows >> shift) != (cols >> shift))
        parts = [mm(full, jnp.where(off, t, 0.0)) for full, t in zip(fulls, ts)]
        fulls = [full - mm(part, full) for full, part in zip(fulls, parts)]
        yield
    result.extend(fulls)


def kernel(s_hbm, l_ref, r_ref, o_hbm, s_ref, o_ref, rt, st, tx, lt, yb, xv, rh, rl, io_sem, send_sem, recv_sem, sh_send, s_send, s_recv, t_send, t_recv, y_send, y_recv):
    me = lax.axis_index("prow")
    col = lax.axis_index("pcol")
    z, x = me // NX, me % NX
    y, c = col // 2, col % 2

    def at_x(k):
        return (z * NX + (x + k + NX) % NX, col)

    def at_z(k):
        return (((z + k + NZ) % NZ) * NX + x, col)

    def at_y(k):
        return (me, ((y + k + NY) % NY) * 2 + c)

    partner = (me, y * 2 + 1 - c)

    s_in = [
        pltpu.make_async_copy(s_hbm.at[:, h, :], s_ref.at[:, h * 128 : (h + 1) * 128], io_sem.at[0]) for h in range(8)
    ]

    def write(d, value):
        for h in range(2):
            o_hbm[pl.ds(2 * d + h, BS, stride=8), :] = value[:, h * 128 : (h + 1) * 128]

    s_in.append(pltpu.make_async_copy(l_ref, lt.at[col], io_sem.at[1]))
    s_in.append(pltpu.make_async_copy(r_ref, rt.at[z, x], io_sem.at[2]))
    for e in s_in:
        e.start()
    barrier = pltpu.get_barrier_semaphore()
    near = [at_x(1), at_x(-1), at_x(2), at_z(1), at_z(-1), at_y(1), at_y(-1), at_y(2), partner]
    for dev in near:
        pl.semaphore_signal(barrier, inc=1, device_id=dev, device_id_type=MESH)
    pl.semaphore_wait(barrier, len(near))

    pltpu.make_async_copy(s_ref, s_ref, io_sem.at[0]).wait()
    s_in[8].wait()
    s_in[9].wait()
    for root in range(2):

        @pl.when(me == root)
        def _():
            st[root, root * 4 : root * 4 + 4] = s_ref[:, root * BS : (root + 1) * BS].reshape(4, 64, BS)
            tx[col, root, root * 16 : root * 16 + 16] = lt[col, root * 16 : root * 16 + 16]

    events = []

    def same(ref, dev, group):
        copy = pltpu.make_async_remote_copy(
            src_ref=ref,
            dst_ref=ref,
            send_sem=send_sem.at[group],
            recv_sem=recv_sem.at[len(events)],
            device_id=dev,
            device_id_type=MESH,
        )
        copy.start()
        events.append(copy)
        return copy

    def all_sent(sem, ref):
        pltpu.make_async_copy(ref, ref, sem).wait()

    def remote(src, dst, ssem, rsem, dev):
        return pltpu.make_async_remote_copy(
            src_ref=src, dst_ref=dst, send_sem=ssem, recv_sem=rsem, device_id=dev, device_id_type=MESH
        )

    dist = jnp.where(z <= NZ // 2, z, NZ - z)
    zdir = jnp.where(z <= NZ // 2, 1, -1)
    passes_on = ((z >= 1) & (z <= 3)) | (z >= 6)

    def s_share(root, k, d):
        return remote(
            s_ref.at[pl.ds(k * 64, 64), pl.ds(d * BS, BS)],
            st.at[d, root * 4 + k],
            sh_send.at[0],
            s_recv.at[0, root * 4 + k],
            (d, col),
        )

    def s_along(k, d, which):
        return remote(st.at[x, k], st.at[x, k], s_send.at[which], s_recv.at[0, k], at_z(d))

    def s_across(k, which):
        return remote(st.at[x, k], st.at[x, k], s_send.at[2], s_recv.at[1, k], at_x(1 - 2 * which))

    def s_over(k):
        d = 1 - 2 * (k % 2)
        part = st.at[(x - d + NX) % NX, k]
        return remote(part, part, s_send.at[3], s_recv.at[2, k], at_x(d))

    def feeds(k):
        return z == 1 + (NZ - 2) * ((k // 2 + k) % 2)

    def s_back(k):
        part = st.at[(x + 2) % NX, k]
        return remote(part, part, s_send.at[4], s_recv.at[2, k], (x, col))

    def s_slot(j):
        turn = j - dist

        @pl.when((turn >= 0) & (turn < 8))
        def _():
            k = turn // 2 + 4 * (turn % 2)

            @pl.when((z != 0) | (x != k // 4))
            def _():
                s_along(k, 1, 0).wait_recv()

            @pl.when(z == 0)
            def _():
                s_along(k, 1, 0).start()
                s_along(k, -1, 1).start()

            @pl.when(passes_on)
            def _():
                s_along(k, zdir, 0).start()

            @pl.when(z != 0)
            def _():
                s_across(k, 0).start()
                s_across(k, 1).start()

        if LAG <= j < LAG + 8:

            @pl.when(z == 0)
            def _():
                k = (j - LAG) // 2 + 4 * ((j - LAG) % 2)
                s_across(k, 0).start()
                s_across(k, 1).start()

        @pl.when((turn >= 2) & (turn < 10) & (z != 0))
        def _():
            k = (turn - 2) // 2 + 4 * ((turn - 2) % 2)
            all_sent(s_recv.at[1, k], st.at[0, 0:2])
            s_over(k).start()

        @pl.when((turn >= 5) & (turn < 13) & (dist == 1))
        def _():
            k = (turn - 5) // 2 + 4 * ((turn - 5) % 2)

            @pl.when(feeds(k))
            def _():
                s_over(k).wait_recv()
                s_back(k).start()

    def s_end():
        @pl.when(z == 0)
        def _():
            for k in range(8):
                all_sent(s_recv.at[1, k], st.at[0, 0:2])

        for k in range(8):

            @pl.when(jnp.logical_not(feeds(k)))
            def _():
                s_over(k).wait_recv()

    def s_sent():
        @pl.when((z == 0) | passes_on)
        def _():
            all_sent(s_send.at[0], st.at[0])

        @pl.when(z == 0)
        def _():
            all_sent(s_send.at[1], st.at[0])

        all_sent(s_send.at[2], st.at[0:2])

        @pl.when(z != 0)
        def _():
            all_sent(s_send.at[3], st.at[0])

        @pl.when(dist == 1)
        def _():
            all_sent(s_send.at[4], st.at[0, 0:4])

    def t_share(root, d):
        return remote(
            lt.at[col, pl.ds(d * 16, 16)],
            tx.at[col, root, pl.ds(d * 16, 16)],
            t_send.at[0],
            t_recv.at[root],
            (d, col),
        )

    quarter = tx.at[col, :, pl.ds(x * 16, 16)]
    t_along = [remote(quarter, quarter, t_send.at[1], t_recv.at[2], at_z(d)) for d in (1, -1, zdir)]
    t_across = [remote(quarter, quarter, t_send.at[2], t_recv.at[3 + w], at_x(d)) for w, d in enumerate((1, -1, 2))]
    t_up = [remote(tx.at[col], tx.at[col], t_send.at[3], t_recv.at[6 + w], at_y(d)) for w, d in enumerate((1, -1, 2))]

    def t_over(w):
        part = tx.at[((y - (0, 1, -1, 2)[w] + NY) % NY) * 2 + c]
        return remote(part, part, t_send.at[4], t_recv.at[9 + w], partner)

    def t_slot(n):
        @pl.when(dist == n)
        def _():
            if n == 0:
                for root in range(2):

                    @pl.when(x != root)
                    def _():
                        t_share(root, x).wait_recv()

                t_along[0].start()
                t_along[1].start()
            else:
                t_along[2].wait_recv()

                @pl.when(passes_on)
                def _():
                    t_along[2].start()

            for e in t_across:
                e.start()

        @pl.when(dist == n - 1)
        def _():
            for e in t_across:
                e.wait_recv()
            for e in t_up:
                e.start()
            t_over(0).start()

    def t_step():
        for w in range(3):
            t_up[w].wait_recv()
            t_over(w + 1).start()

    def t_end():
        for w in range(4):
            t_over(w).wait_recv()

    def t_sent():
        @pl.when(z == 0)
        def _():
            all_sent(t_send.at[1], tx.at[0:2, :, 0:16])

        @pl.when(passes_on)
        def _():
            all_sent(t_send.at[1], tx.at[0, :, 0:16])

        all_sent(t_send.at[2], tx.at[0:3, :, 0:16])
        all_sent(t_send.at[3], tx.at[0:3])
        all_sent(t_send.at[4], tx.at[0:4])

    def t_shares():
        for root in range(2):

            @pl.when(me == root)
            def _():
                for d in range(NX):
                    if d != root:
                        t_share(root, d).start()

    def s_shares(k):
        for root in range(2):

            @pl.when(me == root)
            def _():
                for d in range(NX):
                    if d != root:
                        s_share(root, k, d).start()

    def shares_sent():
        @pl.when(me < 2)
        def _():
            all_sent(t_send.at[0], lt.at[0, 0:48])
            all_sent(sh_send.at[0], st.at[0:3, 0:4])

    class Across:
        def __init__(self, view, plus, minus):
            self.view, self.most = view, {1: plus, -1: minus}
            self.sent = {}

        def on(self, d, s, off):
            src = (z - d * (s - 1) + NZ) % NZ
            self.sent[d, s, off] = same(self.view(src, (x + off + NX) % NX), at_z(d), 0)

        def first(self):
            self.xs = [same(self.view(z, x), at_x(k), 0) for k in (1, -1, 2)]
            for d in (1, -1):
                self.on(d, 1, 0)

        def step(self, s):
            if s == 1:
                for e, k in zip(self.xs, (1, -1, 2)):
                    e.wait_recv()
                    for d in (1, -1):
                        self.on(d, 1, -k)
                return
            for off in (0, -1, 1, -2):
                for d in (1, -1):
                    if (d, s - 1, off) in self.sent:
                        self.sent[d, s - 1, off].wait_recv()
                    if s <= self.most[d]:
                        self.on(d, s, off)

    class Along:
        def __init__(self, view, plus, minus):
            self.view, self.most = view, {1: plus, -1: minus}
            self.zs, self.xs, self.fs = {}, {}, []

        def to_x(self, key, src, d):
            self.xs[key] = (src, d, {k: same(self.view(src, x), at_x(k), 1) for k in (1, -1)})

        def first(self):
            for d in (1, -1):
                self.zs[d, 1] = same(self.view(z, x), at_z(d), 1)
            self.to_x((1, 1), z, 1 if self.most[1] == 4 else -1)

        def step(self, s):
            for d in (1, -1):
                if s > 1 and (d, s - 1) in self.zs:
                    self.zs[d, s - 1].wait_recv()
                    src = (z - d * (s - 1) + NZ) % NZ
                    if s <= self.most[d]:
                        self.zs[d, s] = same(self.view(src, x), at_z(d), 1)
                    self.to_x((d, s), src, d if s < 5 else -d)

        def cross(self, s):
            for d in (1, -1):
                if (d, s) in self.xs:
                    self.forward((d, s))

        def forward(self, key):
            src, d, sent = self.xs[key]
            sent[1].wait_recv()
            sent[-1].wait_recv()
            self.fs.append(same(self.view(src, (x - d + NX) % NX), at_x(d), 1))

        def last(self):
            for e in self.fs:
                e.wait_recv()

    def blocks(first, number):
        def view(zz, xx):
            return rt.at[zz, xx, first : first + number]

        return view

    r_a = Across(blocks(0, R_CUT), 3, 4)
    r_b = Along(blocks(R_CUT, 4 - R_CUT), 3, 4)

    class Panel:
        def __init__(self, ref):
            self.ref = ref

        def first(self):
            self.es = [same(self.ref.at[col], at_y(k), 2) for k in (1, -1, 2)]
            self.ps = [same(self.ref.at[col], partner, 2)]

        def step(self):
            for k, e in zip((1, -1, 2), self.es):
                e.wait_recv()
                self.ps.append(same(self.ref.at[((y - k + NY) % NY) * 2 + c], partner, 2))

        def last(self):
            for e in self.ps:
                e.wait_recv()

    l_p = Panel(lt)

    def panel_of(root):
        return tx[:, root].reshape(512, BS)

    t_shares()
    r_a.first()
    r_b.first()
    l_p.first()
    t_slot(0)
    for k in range(4):
        s_shares(k)
    r_a.step(1)
    r_b.step(2)
    t_slot(1)
    s_slot(0)
    r_b.step(3)
    r_a.step(2)
    t_slot(2)
    s_slot(1)
    r_b.cross(1)
    r_b.step(4)
    t_slot(3)
    s_slot(2)
    r_a.step(3)
    r_b.cross(2)
    t_slot(4)
    s_slot(3)
    r_b.step(5)
    t_slot(5)
    s_slot(4)
    r_b.cross(3)
    r_a.step(4)
    l_p.step()
    s_slot(5)
    t_step()
    r_b.cross(4)
    r_b.cross(5)
    l_p.last()
    t_end()
    r_a.step(5)
    pair = []
    stages = inverse_stages(
        [tx[pl.ds(4 * c, 4), c].reshape(BS, BS).T, rt[pl.ds(4 * c, 4), :, 0].reshape(BS, BS).T], pair
    )
    next(stages)
    s_slot(6)
    next(stages)
    s_slot(7)
    next(stages)
    s_slot(8)
    next(stages)
    s_slot(9)
    next(stages)
    s_slot(10)
    for _ in stages:
        pass
    xv[c] = pair[0]
    xv_copy = same(xv.at[c], partner, 3)
    s_slot(11)
    s_slot(12)
    left1 = panel_of(1)
    t10 = left1[0:BS].T
    mine = lt[...].reshape(512, BS).T
    ri = lax.broadcasted_iota(jnp.int32, (BS, 512), 0)
    ci = lax.broadcasted_iota(jnp.int32, (BS, 512), 1)
    unit = jnp.where(ci == ri + me * BS, -1.0, 0.0)
    a = jnp.where(me < 2, unit, mine)
    xv_copy.wait_recv()
    inv0, inv1 = xv[0], xv[1]
    w1 = mm(a[:, BS:], inv1)
    w0 = mm(a[:, :BS] - mm(w1, t10), inv0)
    wide = halves(jnp.concatenate([w0, w1], axis=1))
    s_slot(13)
    r_b.last()

    def left(d):
        cut = slice(d * BS, (d + 1) * BS)
        base = jnp.where(me < 2, 0.0, s_ref[:, cut])
        o_ref[:, cut] = base - mm3(wide, halves(st[d].reshape(2 * BS, BS)))

    s_end()
    left(0)

    def y_copy(half, dev, k, over):
        part = yb.at[c, pl.ds(half * 128, 128)]
        return pltpu.make_async_remote_copy(
            src_ref=part,
            dst_ref=part,
            send_sem=y_send.at[k],
            recv_sem=y_recv.at[2 * over + half],
            device_id=dev,
            device_id_type=MESH,
        )

    over = [y_copy(h, partner, h, 1) for h in range(2)]
    along = [y_copy(0, at_y(1), 2, 0), y_copy(1, at_y(-1), 3, 0), y_copy(1, at_y(1), 4, 0), y_copy(0, at_y(-1), 5, 0)]

    @pl.when(y == 0)
    def _():
        @pl.when(c == 1)
        def _():
            for e in over:
                e.wait_recv()
            o_ref[:, 0:BS] = o_ref[:, 0:BS] - mm(yb[0], rt[0:4, :, 0].reshape(BS, BS))

        yb[c] = mm(o_ref[:, 0:BS], pair[1].T)
        for e in over:
            e.start()
        for e in along:
            e.start()

    for d in (1, 2, 3):
        left(d)
    for d in range(4):
        high, low = halves(rt[:, :, d].reshape(2 * BS, BS))
        rh[d] = high
        rl[d] = low
    all_sent(send_sem.at[0], s_ref.at[0:248])
    all_sent(send_sem.at[1], s_ref.at[0:248])
    all_sent(send_sem.at[2], lt.at[0:7])
    all_sent(send_sem.at[3], xv.at[0])
    s_sent()
    t_sent()
    shares_sent()

    @pl.when(y == 1)
    def _():
        along[0].wait_recv()
        along[0].start()
        over[0].start()
        along[1].wait_recv()
        over[1].start()

    @pl.when(y == 3)
    def _():
        along[1].wait_recv()
        along[1].start()
        over[1].start()
        along[0].wait_recv()
        over[0].start()

    @pl.when(y == 2)
    def _():
        along[0].wait_recv()
        over[0].start()
        along[1].wait_recv()
        over[1].start()

    def share(which, d):
        rows = pl.ds(pl.multiple_of(which * BS, BS), BS)
        return mm3(halves(yb[which]), (rh[d, rows], rl[d, rows]))

    for d in range(4):
        cut = slice(d * BS, (d + 1) * BS)
        o_ref[:, cut] = o_ref[:, cut] - share(c, d)

    @pl.when((y != 0) | (c == 0))
    def _():
        for e in over:
            e.wait_recv()

    def right(d):
        return o_ref[:, d * BS : (d + 1) * BS] - share(1 - c, d)

    for d in (1, 2, 3):
        write(d, right(d))

    @pl.when(y == 0)
    def _():
        write(0, yb[c])

    @pl.when(y != 0)
    def _():
        write(0, right(0))

    for e in over:
        e.wait_send()

    @pl.when((y == 0) | (y == 1))
    def _():
        along[0].wait_send()

    @pl.when((y == 0) | (y == 3))
    def _():
        along[1].wait_send()

    @pl.when(y == 0)
    def _():
        along[2].wait_send()
        along[3].wait_send()


N_EVENTS = 70


def shards(cross_cov, left_factor, right_factor):
    f32 = jnp.float32
    out = pl.pallas_call(
        kernel,
        out_shape=jax.ShapeDtypeStruct((BS * 8, 128), f32),
        in_specs=[
            pl.BlockSpec(memory_space=pltpu.HBM),
            pl.BlockSpec(memory_space=pltpu.HBM),
            pl.BlockSpec(memory_space=pltpu.HBM),
        ],
        out_specs=pl.BlockSpec(memory_space=pltpu.VMEM),
        scratch_shapes=[
            pltpu.VMEM((BS, 1024), f32),
            pltpu.VMEM((BS, 1024), f32),
            pltpu.VMEM((NZ, NX, 4, 16, BS), f32),
            pltpu.VMEM((4, 8, 64, BS), f32),
            pltpu.VMEM((8, 2, 64, BS), f32),
            pltpu.VMEM((8, 64, 256), f32),
            pltpu.VMEM((2, BS, BS), f32),
            pltpu.VMEM((2, BS, BS), f32),
            pltpu.VMEM((4, 2 * BS, BS), jnp.bfloat16),
            pltpu.VMEM((4, 2 * BS, BS), jnp.bfloat16),
            pltpu.SemaphoreType.DMA((3,)),
            pltpu.SemaphoreType.DMA((4,)),
            pltpu.SemaphoreType.DMA((N_EVENTS,)),
            pltpu.SemaphoreType.DMA((1,)),
            pltpu.SemaphoreType.DMA((5,)),
            pltpu.SemaphoreType.DMA((3, 8)),
            pltpu.SemaphoreType.DMA((5,)),
            pltpu.SemaphoreType.DMA((13,)),
            pltpu.SemaphoreType.DMA((6,)),
            pltpu.SemaphoreType.DMA((4,)),
        ],
        compiler_params=pltpu.CompilerParams(collective_id=0, has_side_effects=True, vmem_limit_bytes=55000000),
    )(
        cross_cov.reshape(BS, 8, 128),
        left_factor.reshape(BS, 64).T,
        jnp.swapaxes(right_factor.reshape(4, BS, 16), 1, 2),
    )
    return out.reshape(cross_cov.shape)


def solution(mesh):
    return jax.shard_map(
        shards,
        mesh=mesh,
        in_specs=(
            P(None, "prow", None, None, "pcol", None),
            P(None, "prow", None, "pcol"),
            P(None, "pcol", None, "prow"),
        ),
        out_specs=P(None, "prow", None, None, "pcol", None),
        check_vma=False,
    )
```

```python
import functools

import jax
import jax.numpy as jnp
from jax import lax
from jax.experimental import pallas as pl
from jax.experimental.pallas import tpu as pltpu
from jax.sharding import PartitionSpec as P

BS = 256
NX = 4
NZ = 8
NY = 4
R_CUT = 2
LAG = 2
MESH = pl.DeviceIdType.MESH


def mm(a, b):
    return jnp.dot(a, b, precision=lax.Precision.HIGHEST, preferred_element_type=jnp.float32)


def halves(a):
    high = a.astype(jnp.bfloat16)
    return high, (a - high.astype(jnp.float32)).astype(jnp.bfloat16)


def mm3(a, b):
    (ah, al), (bh, bl) = a, b

    def dot(p, q):
        return jnp.dot(p, q, preferred_element_type=jnp.float32)

    return dot(ah, bh) + (dot(ah, bl) + dot(al, bh))


def inverse_stages(ts, result):
    n, b = ts[0].shape[0], 32
    m = n // b
    rows = lax.broadcasted_iota(jnp.int32, (n, n), 0)
    cols = lax.broadcasted_iota(jnp.int32, (n, n), 1)
    same = (rows >> 5) == (cols >> 5)
    wide = (
        (lax.broadcasted_iota(jnp.int32, (b, n), 1) & (b - 1)) == lax.broadcasted_iota(jnp.int32, (b, n), 0)
    ).astype(jnp.float32)
    tall = (
        (lax.broadcasted_iota(jnp.int32, (n, b), 0) & (b - 1)) == lax.broadcasted_iota(jnp.int32, (n, b), 1)
    ).astype(jnp.float32)
    ts = [jnp.where(rows >= cols, t, 0.0) for t in ts]
    blocks = jnp.concatenate([mm(jnp.where(same, t, 0.0), tall).reshape(m, b, b) for t in ts], axis=0)
    bi = lax.broadcasted_iota(jnp.int32, blocks.shape, 1)
    bj = lax.broadcasted_iota(jnp.int32, blocks.shape, 2)
    diag = jnp.sum(jnp.where(bi == bj, blocks, 0.0), axis=2, keepdims=True)
    rdiag = 1.0 / diag
    lower = jnp.where(bi > bj, blocks * rdiag, 0.0)
    inv = jnp.where(bi == bj, rdiag, 0.0)
    yield
    for j in range(b - 1):
        inv = inv - lower[:, :, j : j + 1] * inv[:, j : j + 1, :]
        if j == b // 2:
            yield
    fulls = [jnp.where(same, mm(inv[k * m : k * m + m].reshape(n, b), wide), 0.0) for k in range(len(ts))]
    yield
    for shift in (5, 6, 7):
        off = ((rows >> (shift + 1)) == (cols >> (shift + 1))) & ((rows >> shift) != (cols >> shift))
        parts = [mm(full, jnp.where(off, t, 0.0)) for full, t in zip(fulls, ts)]
        fulls = [full - mm(part, full) for full, part in zip(fulls, parts)]
        yield
    result.extend(fulls)


def kernel(s_hbm, l_ref, r_ref, o_hbm, s_ref, o_ref, rt, st, tx, lt, yb, xv, rh, rl, io_sem, send_sem, recv_sem, sh_send, s_send, s_recv, t_send, t_recv, y_send, y_recv):
    me = lax.axis_index("prow")
    col = lax.axis_index("pcol")
    z, x = me // NX, me % NX
    y, c = col // 2, col % 2

    def at_x(k):
        return (z * NX + (x + k + NX) % NX, col)

    def at_z(k):
        return (((z + k + NZ) % NZ) * NX + x, col)

    def at_y(k):
        return (me, ((y + k + NY) % NY) * 2 + c)

    partner = (me, y * 2 + 1 - c)

    s_in = [
        pltpu.make_async_copy(s_hbm.at[:, h, :], s_ref.at[:, h * 128 : (h + 1) * 128], io_sem.at[0]) for h in range(8)
    ]

    def write(d, value):
        for h in range(2):
            o_hbm[pl.ds(2 * d + h, BS, stride=8), :] = value[:, h * 128 : (h + 1) * 128]

    s_in.append(pltpu.make_async_copy(l_ref, lt.at[col], io_sem.at[1]))
    s_in.append(pltpu.make_async_copy(r_ref, rt.at[z, x], io_sem.at[2]))
    for e in s_in:
        e.start()
    barrier = pltpu.get_barrier_semaphore()
    near = [at_x(1), at_x(-1), at_x(2), at_z(1), at_z(-1), at_y(1), at_y(-1), at_y(2), partner]
    for dev in near:
        pl.semaphore_signal(barrier, inc=1, device_id=dev, device_id_type=MESH)
    pl.semaphore_wait(barrier, len(near))

    pltpu.make_async_copy(s_ref, s_ref, io_sem.at[0]).wait()
    s_in[8].wait()
    s_in[9].wait()
    for root in range(2):

        @pl.when(me == root)
        def _():
            st[root, root * 4 : root * 4 + 4] = s_ref[:, root * BS : (root + 1) * BS].reshape(4, 64, BS)
            tx[col, root, root * 16 : root * 16 + 16] = lt[col, root * 16 : root * 16 + 16]

    events = []

    def same(ref, dev, group):
        copy = pltpu.make_async_remote_copy(
            src_ref=ref,
            dst_ref=ref,
            send_sem=send_sem.at[group],
            recv_sem=recv_sem.at[len(events)],
            device_id=dev,
            device_id_type=MESH,
        )
        copy.start()
        events.append(copy)
        return copy

    def all_sent(sem, ref):
        pltpu.make_async_copy(ref, ref, sem).wait()

    def remote(src, dst, ssem, rsem, dev):
        return pltpu.make_async_remote_copy(
            src_ref=src, dst_ref=dst, send_sem=ssem, recv_sem=rsem, device_id=dev, device_id_type=MESH
        )

    dist = jnp.where(z <= NZ // 2, z, NZ - z)
    zdir = jnp.where(z <= NZ // 2, 1, -1)
    passes_on = ((z >= 1) & (z <= 3)) | (z >= 6)

    def s_share(root, k, d):
        return remote(
            s_ref.at[pl.ds(k * 64, 64), pl.ds(d * BS, BS)],
            st.at[d, root * 4 + k],
            sh_send.at[0],
            s_recv.at[0, root * 4 + k],
            (d, col),
        )

    def s_along(k, d, which):
        return remote(st.at[x, k], st.at[x, k], s_send.at[which], s_recv.at[0, k], at_z(d))

    def s_across(k, which):
        return remote(st.at[x, k], st.at[x, k], s_send.at[2], s_recv.at[1, k], at_x(1 - 2 * which))

    def s_over(k):
        d = 1 - 2 * (k % 2)
        part = st.at[(x - d + NX) % NX, k]
        return remote(part, part, s_send.at[3], s_recv.at[2, k], at_x(d))

    def feeds(k):
        return z == 1 + (NZ - 2) * ((k // 2 + k) % 2)

    def s_back(k):
        part = st.at[(x + 2) % NX, k]
        return remote(part, part, s_send.at[4], s_recv.at[2, k], (x, col))

    def s_slot(j):
        turn = j - dist

        @pl.when((turn >= 0) & (turn < 8))
        def _():
            k = turn // 2 + 4 * (turn % 2)

            @pl.when((z != 0) | (x != k // 4))
            def _():
                s_along(k, 1, 0).wait_recv()

            @pl.when(z == 0)
            def _():
                s_along(k, 1, 0).start()
                s_along(k, -1, 1).start()

            @pl.when(passes_on)
            def _():
                s_along(k, zdir, 0).start()

            @pl.when(z != 0)
            def _():
                s_across(k, 0).start()
                s_across(k, 1).start()

        if LAG <= j < LAG + 8:

            @pl.when(z == 0)
            def _():
                k = (j - LAG) // 2 + 4 * ((j - LAG) % 2)
                s_across(k, 0).start()
                s_across(k, 1).start()

        @pl.when((turn >= 2) & (turn < 10) & (z != 0))
        def _():
            k = (turn - 2) // 2 + 4 * ((turn - 2) % 2)
            all_sent(s_recv.at[1, k], st.at[0, 0:2])
            s_over(k).start()

        @pl.when((turn >= 5) & (turn < 13) & (dist == 1))
        def _():
            k = (turn - 5) // 2 + 4 * ((turn - 5) % 2)

            @pl.when(feeds(k))
            def _():
                s_over(k).wait_recv()
                s_back(k).start()

    def s_end():
        @pl.when(z == 0)
        def _():
            for k in range(8):
                all_sent(s_recv.at[1, k], st.at[0, 0:2])

        for k in range(8):

            @pl.when(jnp.logical_not(feeds(k)))
            def _():
                s_over(k).wait_recv()

    def s_sent():
        @pl.when((z == 0) | passes_on)
        def _():
            all_sent(s_send.at[0], st.at[0])

        @pl.when(z == 0)
        def _():
            all_sent(s_send.at[1], st.at[0])

        all_sent(s_send.at[2], st.at[0:2])

        @pl.when(z != 0)
        def _():
            all_sent(s_send.at[3], st.at[0])

        @pl.when(dist == 1)
        def _():
            all_sent(s_send.at[4], st.at[0, 0:4])

    def t_share(root, d):
        return remote(
            lt.at[col, pl.ds(d * 16, 16)],
            tx.at[col, root, pl.ds(d * 16, 16)],
            t_send.at[0],
            t_recv.at[root],
            (d, col),
        )

    quarter = tx.at[col, :, pl.ds(x * 16, 16)]
    t_along = [remote(quarter, quarter, t_send.at[1], t_recv.at[2], at_z(d)) for d in (1, -1, zdir)]
    t_across = [remote(quarter, quarter, t_send.at[2], t_recv.at[3 + w], at_x(d)) for w, d in enumerate((1, -1, 2))]
    t_up = [remote(tx.at[col], tx.at[col], t_send.at[3], t_recv.at[6 + w], at_y(d)) for w, d in enumerate((1, -1, 2))]

    def t_over(w):
        part = tx.at[((y - (0, 1, -1, 2)[w] + NY) % NY) * 2 + c]
        return remote(part, part, t_send.at[4], t_recv.at[9 + w], partner)

    def t_slot(n):
        @pl.when(dist == n)
        def _():
            if n == 0:
                for root in range(2):

                    @pl.when(x != root)
                    def _():
                        t_share(root, x).wait_recv()

                t_along[0].start()
                t_along[1].start()
            else:
                t_along[2].wait_recv()

                @pl.when(passes_on)
                def _():
                    t_along[2].start()

            for e in t_across:
                e.start()

        @pl.when(dist == n - 1)
        def _():
            for e in t_across:
                e.wait_recv()
            for e in t_up:
                e.start()
            t_over(0).start()

    def t_step():
        for w in range(3):
            t_up[w].wait_recv()
            t_over(w + 1).start()

    def t_end():
        for w in range(4):
            t_over(w).wait_recv()

    def t_sent():
        @pl.when(z == 0)
        def _():
            all_sent(t_send.at[1], tx.at[0:2, :, 0:16])

        @pl.when(passes_on)
        def _():
            all_sent(t_send.at[1], tx.at[0, :, 0:16])

        all_sent(t_send.at[2], tx.at[0:3, :, 0:16])
        all_sent(t_send.at[3], tx.at[0:3])
        all_sent(t_send.at[4], tx.at[0:4])

    def t_shares():
        for root in range(2):

            @pl.when(me == root)
            def _():
                for d in range(NX):
                    if d != root:
                        t_share(root, d).start()

    def s_shares(k):
        for root in range(2):

            @pl.when(me == root)
            def _():
                for d in range(NX):
                    if d != root:
                        s_share(root, k, d).start()

    def shares_sent():
        @pl.when(me < 2)
        def _():
            all_sent(t_send.at[0], lt.at[0, 0:48])
            all_sent(sh_send.at[0], st.at[0:3, 0:4])

    class Across:
        def __init__(self, view, plus, minus):
            self.view, self.most = view, {1: plus, -1: minus}
            self.sent = {}

        def on(self, d, s, off):
            src = (z - d * (s - 1) + NZ) % NZ
            self.sent[d, s, off] = same(self.view(src, (x + off + NX) % NX), at_z(d), 0)

        def first(self):
            self.xs = [same(self.view(z, x), at_x(k), 0) for k in (1, -1, 2)]
            for d in (1, -1):
                self.on(d, 1, 0)

        def step(self, s):
            if s == 1:
                for e, k in zip(self.xs, (1, -1, 2)):
                    e.wait_recv()
                    for d in (1, -1):
                        self.on(d, 1, -k)
                return
            for off in (0, -1, 1, -2):
                for d in (1, -1):
                    if (d, s - 1, off) in self.sent:
                        self.sent[d, s - 1, off].wait_recv()
                    if s <= self.most[d]:
                        self.on(d, s, off)

    class Along:
        def __init__(self, view, plus, minus):
            self.view, self.most = view, {1: plus, -1: minus}
            self.zs, self.xs, self.fs = {}, {}, []

        def to_x(self, key, src, d):
            self.xs[key] = (src, d, {k: same(self.view(src, x), at_x(k), 1) for k in (1, -1)})

        def first(self):
            for d in (1, -1):
                self.zs[d, 1] = same(self.view(z, x), at_z(d), 1)
            self.to_x((1, 1), z, 1 if self.most[1] == 4 else -1)

        def step(self, s):
            for d in (1, -1):
                if s > 1 and (d, s - 1) in self.zs:
                    self.zs[d, s - 1].wait_recv()
                    src = (z - d * (s - 1) + NZ) % NZ
                    if s <= self.most[d]:
                        self.zs[d, s] = same(self.view(src, x), at_z(d), 1)
                    self.to_x((d, s), src, d if s < 5 else -d)

        def cross(self, s):
            for d in (1, -1):
                if (d, s) in self.xs:
                    self.forward((d, s))

        def forward(self, key):
            src, d, sent = self.xs[key]
            sent[1].wait_recv()
            sent[-1].wait_recv()
            self.fs.append(same(self.view(src, (x - d + NX) % NX), at_x(d), 1))

        def last(self):
            for e in self.fs:
                e.wait_recv()

    def blocks(first, number):
        def view(zz, xx):
            return rt.at[zz, xx, first : first + number]

        return view

    r_a = Across(blocks(0, R_CUT), 3, 4)
    r_b = Along(blocks(R_CUT, 4 - R_CUT), 3, 4)

    class Panel:
        def __init__(self, ref):
            self.ref = ref

        def first(self):
            self.es = [same(self.ref.at[col], at_y(k), 2) for k in (1, -1, 2)]
            self.ps = [same(self.ref.at[col], partner, 2)]

        def step(self):
            for k, e in zip((1, -1, 2), self.es):
                e.wait_recv()
                self.ps.append(same(self.ref.at[((y - k + NY) % NY) * 2 + c], partner, 2))

        def last(self):
            for e in self.ps:
                e.wait_recv()

    l_p = Panel(lt)

    def panel_of(root):
        return tx[:, root].reshape(512, BS)

    t_shares()
    r_a.first()
    r_b.first()
    l_p.first()
    t_slot(0)
    for k in range(4):
        s_shares(k)
    r_a.step(1)
    r_b.step(2)
    t_slot(1)
    s_slot(0)
    r_b.step(3)
    r_a.step(2)
    t_slot(2)
    s_slot(1)
    r_b.cross(1)
    r_b.step(4)
    t_slot(3)
    s_slot(2)
    r_a.step(3)
    r_b.cross(2)
    t_slot(4)
    s_slot(3)
    r_b.step(5)
    t_slot(5)
    s_slot(4)
    r_b.cross(3)
    r_a.step(4)
    l_p.step()
    s_slot(5)
    t_step()
    r_b.cross(4)
    r_b.cross(5)
    l_p.last()
    t_end()
    r_a.step(5)
    pair = []
    stages = inverse_stages(
        [tx[pl.ds(4 * c, 4), c].reshape(BS, BS).T, rt[pl.ds(4 * c, 4), :, 0].reshape(BS, BS).T], pair
    )
    next(stages)
    s_slot(6)
    next(stages)
    s_slot(7)
    next(stages)
    s_slot(8)
    next(stages)
    s_slot(9)
    next(stages)
    s_slot(10)
    for _ in stages:
        pass
    xv[c] = pair[0]
    xv_copy = same(xv.at[c], partner, 3)
    s_slot(11)
    s_slot(12)
    left1 = panel_of(1)
    t10 = left1[0:BS].T
    mine = lt[...].reshape(512, BS).T
    ri = lax.broadcasted_iota(jnp.int32, (BS, 512), 0)
    ci = lax.broadcasted_iota(jnp.int32, (BS, 512), 1)
    unit = jnp.where(ci == ri + me * BS, -1.0, 0.0)
    a = jnp.where(me < 2, unit, mine)
    xv_copy.wait_recv()
    inv0, inv1 = xv[0], xv[1]
    w1 = mm(a[:, BS:], inv1)
    w0 = mm(a[:, :BS] - mm(w1, t10), inv0)
    wide = halves(jnp.concatenate([w0, w1], axis=1))
    s_slot(13)
    r_b.last()

    def left(d):
        cut = slice(d * BS, (d + 1) * BS)
        base = jnp.where(me < 2, 0.0, s_ref[:, cut])
        o_ref[:, cut] = base - mm3(wide, halves(st[d].reshape(2 * BS, BS)))

    s_end()
    left(0)

    def y_copy(half, dev, k, over):
        part = yb.at[c, pl.ds(half * 64, 64)]
        return pltpu.make_async_remote_copy(
            src_ref=part,
            dst_ref=part,
            send_sem=y_send.at[k],
            recv_sem=y_recv.at[4 * over + half],
            device_id=dev,
            device_id_type=MESH,
        )

    over = [y_copy(q, partner, q, 1) for q in range(4)]
    up = [y_copy(q, at_y(1), 4 + q, 0) for q in range(4)]
    down = [y_copy(q, at_y(-1), 8 + q, 0) for q in range(4)]

    @pl.when(y == 0)
    def _():
        @pl.when(c == 1)
        def _():
            for e in over:
                e.wait_recv()
            o_ref[:, 0:BS] = o_ref[:, 0:BS] - mm(yb[0], rt[0:4, :, 0].reshape(BS, BS))

        yb[c] = mm(o_ref[:, 0:BS], pair[1].T)
        for e in over:
            e.start()
        for q in range(4):
            up[q].start()
            down[(q + 2) % 4].start()

    for d in (1, 2, 3):
        left(d)
    for d in range(4):
        high, low = halves(rt[:, :, d].reshape(2 * BS, BS))
        rh[d] = high
        rl[d] = low
    all_sent(send_sem.at[0], s_ref.at[0:248])
    all_sent(send_sem.at[1], s_ref.at[0:248])
    all_sent(send_sem.at[2], lt.at[0:7])
    all_sent(send_sem.at[3], xv.at[0])
    s_sent()
    t_sent()
    shares_sent()

    def relay(order, onward):
        for q in order:
            up[q].wait_recv()
            if q in onward:
                onward[q].start()
            over[q].start()

    @pl.when(y == 1)
    def _():
        relay((0, 1, 2, 3), {0: up[0], 1: up[1]})

    @pl.when(y == 3)
    def _():
        relay((2, 3, 0, 1), {2: down[2], 3: down[3]})

    @pl.when(y == 2)
    def _():
        relay((0, 2, 1, 3), {})

    def share(which, d):
        rows = pl.ds(pl.multiple_of(which * BS, BS), BS)
        return mm3(halves(yb[which]), (rh[d, rows], rl[d, rows]))

    for d in range(4):
        cut = slice(d * BS, (d + 1) * BS)
        o_ref[:, cut] = o_ref[:, cut] - share(c, d)

    @pl.when((y != 0) | (c == 0))
    def _():
        for e in over:
            e.wait_recv()

    def right(d):
        return o_ref[:, d * BS : (d + 1) * BS] - share(1 - c, d)

    for d in (1, 2, 3):
        write(d, right(d))

    @pl.when(y == 0)
    def _():
        write(0, yb[c])

    @pl.when(y != 0)
    def _():
        write(0, right(0))

    for e in over:
        e.wait_send()

    @pl.when((y == 0) | (y == 1))
    def _():
        up[0].wait_send()
        up[1].wait_send()

    @pl.when((y == 0) | (y == 3))
    def _():
        down[2].wait_send()
        down[3].wait_send()

    @pl.when(y == 0)
    def _():
        for e in (up[2], up[3], down[0], down[1]):
            e.wait_send()


N_EVENTS = 70


def shards(cross_cov, left_factor, right_factor):
    f32 = jnp.float32
    out = pl.pallas_call(
        kernel,
        out_shape=jax.ShapeDtypeStruct((BS * 8, 128), f32),
        in_specs=[
            pl.BlockSpec(memory_space=pltpu.HBM),
            pl.BlockSpec(memory_space=pltpu.HBM),
            pl.BlockSpec(memory_space=pltpu.HBM),
        ],
        out_specs=pl.BlockSpec(memory_space=pltpu.VMEM),
        scratch_shapes=[
            pltpu.VMEM((BS, 1024), f32),
            pltpu.VMEM((BS, 1024), f32),
            pltpu.VMEM((NZ, NX, 4, 16, BS), f32),
            pltpu.VMEM((4, 8, 64, BS), f32),
            pltpu.VMEM((8, 2, 64, BS), f32),
            pltpu.VMEM((8, 64, 256), f32),
            pltpu.VMEM((2, BS, BS), f32),
            pltpu.VMEM((2, BS, BS), f32),
            pltpu.VMEM((4, 2 * BS, BS), jnp.bfloat16),
            pltpu.VMEM((4, 2 * BS, BS), jnp.bfloat16),
            pltpu.SemaphoreType.DMA((3,)),
            pltpu.SemaphoreType.DMA((4,)),
            pltpu.SemaphoreType.DMA((N_EVENTS,)),
            pltpu.SemaphoreType.DMA((1,)),
            pltpu.SemaphoreType.DMA((5,)),
            pltpu.SemaphoreType.DMA((3, 8)),
            pltpu.SemaphoreType.DMA((5,)),
            pltpu.SemaphoreType.DMA((13,)),
            pltpu.SemaphoreType.DMA((12,)),
            pltpu.SemaphoreType.DMA((8,)),
        ],
        compiler_params=pltpu.CompilerParams(collective_id=0, has_side_effects=True, vmem_limit_bytes=55000000),
    )(
        cross_cov.reshape(BS, 8, 128),
        left_factor.reshape(BS, 64).T,
        jnp.swapaxes(right_factor.reshape(4, BS, 16), 1, 2),
    )
    return out.reshape(cross_cov.shape)


def solution(mesh):
    return jax.shard_map(
        shards,
        mesh=mesh,
        in_specs=(
            P(None, "prow", None, None, "pcol", None),
            P(None, "prow", None, "pcol"),
            P(None, "pcol", None, "prow"),
        ),
        out_specs=P(None, "prow", None, None, "pcol", None),
        check_vma=False,
    )
```

```python
import functools

import jax
import jax.numpy as jnp
from jax import lax
from jax.experimental import pallas as pl
from jax.experimental.pallas import tpu as pltpu
from jax.sharding import PartitionSpec as P

BS = 256
NX = 4
NZ = 8
NY = 4
R_CUT = 2
LAG = 3
MESH = pl.DeviceIdType.MESH


def mm(a, b):
    return jnp.dot(a, b, precision=lax.Precision.HIGHEST, preferred_element_type=jnp.float32)


def halves(a):
    high = a.astype(jnp.bfloat16)
    return high, (a - high.astype(jnp.float32)).astype(jnp.bfloat16)


def mm3(a, b):
    (ah, al), (bh, bl) = a, b

    def dot(p, q):
        return jnp.dot(p, q, preferred_element_type=jnp.float32)

    return dot(ah, bh) + (dot(ah, bl) + dot(al, bh))


def inverse_stages(ts, result):
    n, b = ts[0].shape[0], 32
    m = n // b
    rows = lax.broadcasted_iota(jnp.int32, (n, n), 0)
    cols = lax.broadcasted_iota(jnp.int32, (n, n), 1)
    same = (rows >> 5) == (cols >> 5)
    wide = (
        (lax.broadcasted_iota(jnp.int32, (b, n), 1) & (b - 1)) == lax.broadcasted_iota(jnp.int32, (b, n), 0)
    ).astype(jnp.float32)
    tall = (
        (lax.broadcasted_iota(jnp.int32, (n, b), 0) & (b - 1)) == lax.broadcasted_iota(jnp.int32, (n, b), 1)
    ).astype(jnp.float32)
    ts = [jnp.where(rows >= cols, t, 0.0) for t in ts]
    blocks = jnp.concatenate([mm(jnp.where(same, t, 0.0), tall).reshape(m, b, b) for t in ts], axis=0)
    bi = lax.broadcasted_iota(jnp.int32, blocks.shape, 1)
    bj = lax.broadcasted_iota(jnp.int32, blocks.shape, 2)
    diag = jnp.sum(jnp.where(bi == bj, blocks, 0.0), axis=2, keepdims=True)
    rdiag = 1.0 / diag
    lower = jnp.where(bi > bj, blocks * rdiag, 0.0)
    inv = jnp.where(bi == bj, rdiag, 0.0)
    yield
    for j in range(b - 1):
        inv = inv - lower[:, :, j : j + 1] * inv[:, j : j + 1, :]
        if j == b // 2:
            yield
    fulls = [jnp.where(same, mm(inv[k * m : k * m + m].reshape(n, b), wide), 0.0) for k in range(len(ts))]
    yield
    for shift in (5, 6, 7):
        off = ((rows >> (shift + 1)) == (cols >> (shift + 1))) & ((rows >> shift) != (cols >> shift))
        parts = [mm(full, jnp.where(off, t, 0.0)) for full, t in zip(fulls, ts)]
        fulls = [full - mm(part, full) for full, part in zip(fulls, parts)]
        yield
    result.extend(fulls)


def kernel(s_hbm, l_ref, r_ref, o_hbm, s_ref, o_ref, rt, st, tx, lt, yb, xv, rh, rl, io_sem, send_sem, recv_sem, sh_send, s_send, s_recv, t_send, t_recv, y_send, y_recv):
    me = lax.axis_index("prow")
    col = lax.axis_index("pcol")
    z, x = me // NX, me % NX
    y, c = col // 2, col % 2

    def at_x(k):
        return (z * NX + (x + k + NX) % NX, col)

    def at_z(k):
        return (((z + k + NZ) % NZ) * NX + x, col)

    def at_y(k):
        return (me, ((y + k + NY) % NY) * 2 + c)

    partner = (me, y * 2 + 1 - c)

    s_in = [
        pltpu.make_async_copy(s_hbm.at[:, h, :], s_ref.at[:, h * 128 : (h + 1) * 128], io_sem.at[0]) for h in range(8)
    ]

    def write(d, value):
        for h in range(2):
            o_hbm[pl.ds(2 * d + h, BS, stride=8), :] = value[:, h * 128 : (h + 1) * 128]

    s_in.append(pltpu.make_async_copy(l_ref, lt.at[col], io_sem.at[1]))
    s_in.append(pltpu.make_async_copy(r_ref, rt.at[z, x], io_sem.at[2]))
    for e in s_in:
        e.start()
    barrier = pltpu.get_barrier_semaphore()
    near = [at_x(1), at_x(-1), at_x(2), at_z(1), at_z(-1), at_y(1), at_y(-1), at_y(2), partner]
    for dev in near:
        pl.semaphore_signal(barrier, inc=1, device_id=dev, device_id_type=MESH)
    pl.semaphore_wait(barrier, len(near))

    pltpu.make_async_copy(s_ref, s_ref, io_sem.at[0]).wait()
    s_in[8].wait()
    s_in[9].wait()
    for root in range(2):

        @pl.when(me == root)
        def _():
            st[root, root * 4 : root * 4 + 4] = s_ref[:, root * BS : (root + 1) * BS].reshape(4, 64, BS)
            tx[col, root, root * 16 : root * 16 + 16] = lt[col, root * 16 : root * 16 + 16]

    events = []

    def same(ref, dev, group):
        copy = pltpu.make_async_remote_copy(
            src_ref=ref,
            dst_ref=ref,
            send_sem=send_sem.at[group],
            recv_sem=recv_sem.at[len(events)],
            device_id=dev,
            device_id_type=MESH,
        )
        copy.start()
        events.append(copy)
        return copy

    def all_sent(sem, ref):
        pltpu.make_async_copy(ref, ref, sem).wait()

    def remote(src, dst, ssem, rsem, dev):
        return pltpu.make_async_remote_copy(
            src_ref=src, dst_ref=dst, send_sem=ssem, recv_sem=rsem, device_id=dev, device_id_type=MESH
        )

    dist = jnp.where(z <= NZ // 2, z, NZ - z)
    zdir = jnp.where(z <= NZ // 2, 1, -1)
    passes_on = ((z >= 1) & (z <= 3)) | (z >= 6)

    def s_share(root, k, d):
        return remote(
            s_ref.at[pl.ds(k * 64, 64), pl.ds(d * BS, BS)],
            st.at[d, root * 4 + k],
            sh_send.at[0],
            s_recv.at[0, root * 4 + k],
            (d, col),
        )

    def s_along(k, d, which):
        return remote(st.at[x, k], st.at[x, k], s_send.at[which], s_recv.at[0, k], at_z(d))

    def s_across(k, which):
        return remote(st.at[x, k], st.at[x, k], s_send.at[2], s_recv.at[1, k], at_x(1 - 2 * which))

    def s_over(k):
        d = 1 - 2 * (k % 2)
        part = st.at[(x - d + NX) % NX, k]
        return remote(part, part, s_send.at[3], s_recv.at[2, k], at_x(d))

    def feeds(k):
        return z == 1 + (NZ - 2) * ((k // 2 + k) % 2)

    def s_back(k):
        part = st.at[(x + 2) % NX, k]
        return remote(part, part, s_send.at[4], s_recv.at[2, k], (x, col))

    def s_slot(j):
        turn = j - dist

        @pl.when((turn >= 0) & (turn < 8))
        def _():
            k = turn // 2 + 4 * (turn % 2)

            @pl.when((z != 0) | (x != k // 4))
            def _():
                s_along(k, 1, 0).wait_recv()

            @pl.when(z == 0)
            def _():
                s_along(k, 1, 0).start()
                s_along(k, -1, 1).start()

            @pl.when(passes_on)
            def _():
                s_along(k, zdir, 0).start()

            @pl.when(z != 0)
            def _():
                s_across(k, 0).start()
                s_across(k, 1).start()

        if LAG <= j < LAG + 8:

            @pl.when(z == 0)
            def _():
                k = (j - LAG) // 2 + 4 * ((j - LAG) % 2)
                s_across(k, 0).start()
                s_across(k, 1).start()

        @pl.when((turn >= 2) & (turn < 10) & (z != 0))
        def _():
            k = (turn - 2) // 2 + 4 * ((turn - 2) % 2)
            all_sent(s_recv.at[1, k], st.at[0, 0:2])
            s_over(k).start()

        @pl.when((turn >= 5) & (turn < 13) & (dist == 1))
        def _():
            k = (turn - 5) // 2 + 4 * ((turn - 5) % 2)

            @pl.when(feeds(k))
            def _():
                s_over(k).wait_recv()
                s_back(k).start()

    def s_end():
        @pl.when(z == 0)
        def _():
            for k in range(8):
                all_sent(s_recv.at[1, k], st.at[0, 0:2])

        for k in range(8):

            @pl.when(jnp.logical_not(feeds(k)))
            def _():
                s_over(k).wait_recv()

    def s_sent():
        @pl.when((z == 0) | passes_on)
        def _():
            all_sent(s_send.at[0], st.at[0])

        @pl.when(z == 0)
        def _():
            all_sent(s_send.at[1], st.at[0])

        all_sent(s_send.at[2], st.at[0:2])

        @pl.when(z != 0)
        def _():
            all_sent(s_send.at[3], st.at[0])

        @pl.when(dist == 1)
        def _():
            all_sent(s_send.at[4], st.at[0, 0:4])

    def t_share(root, d):
        return remote(
            lt.at[col, pl.ds(d * 16, 16)],
            tx.at[col, root, pl.ds(d * 16, 16)],
            t_send.at[0],
            t_recv.at[root],
            (d, col),
        )

    quarter = tx.at[col, :, pl.ds(x * 16, 16)]
    t_along = [remote(quarter, quarter, t_send.at[1], t_recv.at[2], at_z(d)) for d in (1, -1, zdir)]
    t_across = [remote(quarter, quarter, t_send.at[2], t_recv.at[3 + w], at_x(d)) for w, d in enumerate((1, -1, 2))]
    t_up = [remote(tx.at[col], tx.at[col], t_send.at[3], t_recv.at[6 + w], at_y(d)) for w, d in enumerate((1, -1, 2))]

    def t_over(w):
        part = tx.at[((y - (0, 1, -1, 2)[w] + NY) % NY) * 2 + c]
        return remote(part, part, t_send.at[4], t_recv.at[9 + w], partner)

    def t_slot(n):
        @pl.when(dist == n)
        def _():
            if n == 0:
                for root in range(2):

                    @pl.when(x != root)
                    def _():
                        t_share(root, x).wait_recv()

                t_along[0].start()
                t_along[1].start()
            else:
                t_along[2].wait_recv()

                @pl.when(passes_on)
                def _():
                    t_along[2].start()

            for e in t_across:
                e.start()

        @pl.when(dist == n - 1)
        def _():
            for e in t_across:
                e.wait_recv()
            for e in t_up:
                e.start()
            t_over(0).start()

    def t_step():
        for w in range(3):
            t_up[w].wait_recv()
            t_over(w + 1).start()

    def t_end():
        for w in range(4):
            t_over(w).wait_recv()

    def t_sent():
        @pl.when(z == 0)
        def _():
            all_sent(t_send.at[1], tx.at[0:2, :, 0:16])

        @pl.when(passes_on)
        def _():
            all_sent(t_send.at[1], tx.at[0, :, 0:16])

        all_sent(t_send.at[2], tx.at[0:3, :, 0:16])
        all_sent(t_send.at[3], tx.at[0:3])
        all_sent(t_send.at[4], tx.at[0:4])

    def t_shares():
        for root in range(2):

            @pl.when(me == root)
            def _():
                for d in range(NX):
                    if d != root:
                        t_share(root, d).start()

    def s_shares(k):
        for root in range(2):

            @pl.when(me == root)
            def _():
                for d in range(NX):
                    if d != root:
                        s_share(root, k, d).start()

    def shares_sent():
        @pl.when(me < 2)
        def _():
            all_sent(t_send.at[0], lt.at[0, 0:48])
            all_sent(sh_send.at[0], st.at[0:3, 0:4])

    class Across:
        def __init__(self, view, plus, minus):
            self.view, self.most = view, {1: plus, -1: minus}
            self.sent = {}

        def on(self, d, s, off):
            src = (z - d * (s - 1) + NZ) % NZ
            self.sent[d, s, off] = same(self.view(src, (x + off + NX) % NX), at_z(d), 0)

        def first(self):
            self.xs = [same(self.view(z, x), at_x(k), 0) for k in (1, -1, 2)]
            for d in (1, -1):
                self.on(d, 1, 0)

        def step(self, s):
            if s == 1:
                for e, k in zip(self.xs, (1, -1, 2)):
                    e.wait_recv()
                    for d in (1, -1):
                        self.on(d, 1, -k)
                return
            for off in (0, -1, 1, -2):
                for d in (1, -1):
                    if (d, s - 1, off) in self.sent:
                        self.sent[d, s - 1, off].wait_recv()
                    if s <= self.most[d]:
                        self.on(d, s, off)

    class Along:
        def __init__(self, view, plus, minus):
            self.view, self.most = view, {1: plus, -1: minus}
            self.zs, self.xs, self.fs = {}, {}, []

        def to_x(self, key, src, d):
            self.xs[key] = (src, d, {k: same(self.view(src, x), at_x(k), 1) for k in (1, -1)})

        def first(self):
            for d in (1, -1):
                self.zs[d, 1] = same(self.view(z, x), at_z(d), 1)
            self.to_x((1, 1), z, 1 if self.most[1] == 4 else -1)

        def step(self, s):
            for d in (1, -1):
                if s > 1 and (d, s - 1) in self.zs:
                    self.zs[d, s - 1].wait_recv()
                    src = (z - d * (s - 1) + NZ) % NZ
                    if s <= self.most[d]:
                        self.zs[d, s] = same(self.view(src, x), at_z(d), 1)
                    self.to_x((d, s), src, d if s < 5 else -d)

        def cross(self, s):
            for d in (1, -1):
                if (d, s) in self.xs:
                    self.forward((d, s))

        def forward(self, key):
            src, d, sent = self.xs[key]
            sent[1].wait_recv()
            sent[-1].wait_recv()
            self.fs.append(same(self.view(src, (x - d + NX) % NX), at_x(d), 1))

        def last(self):
            for e in self.fs:
                e.wait_recv()

    def blocks(first, number):
        def view(zz, xx):
            return rt.at[zz, xx, first : first + number]

        return view

    r_a = Across(blocks(0, R_CUT), 3, 4)
    r_b = Along(blocks(R_CUT, 4 - R_CUT), 3, 4)

    class Panel:
        def __init__(self, ref):
            self.ref = ref

        def first(self):
            self.es = [same(self.ref.at[col], at_y(k), 2) for k in (1, -1, 2)]
            self.ps = [same(self.ref.at[col], partner, 2)]

        def step(self):
            for k, e in zip((1, -1, 2), self.es):
                e.wait_recv()
                self.ps.append(same(self.ref.at[((y - k + NY) % NY) * 2 + c], partner, 2))

        def last(self):
            for e in self.ps:
                e.wait_recv()

    l_p = Panel(lt)

    def panel_of(root):
        return tx[:, root].reshape(512, BS)

    t_shares()
    r_a.first()
    r_b.first()
    l_p.first()
    t_slot(0)
    for k in range(4):
        s_shares(k)
    r_a.step(1)
    r_b.step(2)
    t_slot(1)
    s_slot(0)
    r_b.step(3)
    r_a.step(2)
    t_slot(2)
    s_slot(1)
    r_b.cross(1)
    r_b.step(4)
    t_slot(3)
    s_slot(2)
    r_a.step(3)
    r_b.cross(2)
    t_slot(4)
    s_slot(3)
    r_b.step(5)
    t_slot(5)
    s_slot(4)
    r_b.cross(3)
    r_a.step(4)
    l_p.step()
    s_slot(5)
    t_step()
    r_b.cross(4)
    r_b.cross(5)
    l_p.last()
    t_end()
    r_a.step(5)
    pair = []
    stages = inverse_stages(
        [tx[pl.ds(4 * c, 4), c].reshape(BS, BS).T, rt[pl.ds(4 * c, 4), :, 0].reshape(BS, BS).T], pair
    )
    next(stages)
    s_slot(6)
    next(stages)
    s_slot(7)
    next(stages)
    s_slot(8)
    next(stages)
    s_slot(9)
    next(stages)
    s_slot(10)
    for _ in stages:
        pass
    xv[c] = pair[0]
    xv_copy = same(xv.at[c], partner, 3)
    s_slot(11)
    s_slot(12)
    left1 = panel_of(1)
    t10 = left1[0:BS].T
    mine = lt[...].reshape(512, BS).T
    ri = lax.broadcasted_iota(jnp.int32, (BS, 512), 0)
    ci = lax.broadcasted_iota(jnp.int32, (BS, 512), 1)
    unit = jnp.where(ci == ri + me * BS, -1.0, 0.0)
    a = jnp.where(me < 2, unit, mine)
    xv_copy.wait_recv()
    inv0, inv1 = xv[0], xv[1]
    w1 = mm(a[:, BS:], inv1)
    w0 = mm(a[:, :BS] - mm(w1, t10), inv0)
    wide = halves(jnp.concatenate([w0, w1], axis=1))
    s_slot(13)
    r_b.last()

    def left(d):
        cut = slice(d * BS, (d + 1) * BS)
        base = jnp.where(me < 2, 0.0, s_ref[:, cut])
        o_ref[:, cut] = base - mm3(wide, halves(st[d].reshape(2 * BS, BS)))

    s_end()
    left(0)

    def y_copy(half, dev, k, over):
        part = yb.at[c, pl.ds(half * 64, 64)]
        return pltpu.make_async_remote_copy(
            src_ref=part,
            dst_ref=part,
            send_sem=y_send.at[k],
            recv_sem=y_recv.at[4 * over + half],
            device_id=dev,
            device_id_type=MESH,
        )

    over = [y_copy(q, partner, q, 1) for q in range(4)]
    up = [y_copy(q, at_y(1), 4 + q, 0) for q in range(4)]
    down = [y_copy(q, at_y(-1), 8 + q, 0) for q in range(4)]

    @pl.when(y == 0)
    def _():
        @pl.when(c == 1)
        def _():
            for e in over:
                e.wait_recv()
            o_ref[:, 0:BS] = o_ref[:, 0:BS] - mm(yb[0], rt[0:4, :, 0].reshape(BS, BS))

        yb[c] = mm(o_ref[:, 0:BS], pair[1].T)
        for e in over:
            e.start()
        for q in range(4):
            up[q].start()
            down[(q + 2) % 4].start()

    for d in (1, 2, 3):
        left(d)
    for d in range(4):
        high, low = halves(rt[:, :, d].reshape(2 * BS, BS))
        rh[d] = high
        rl[d] = low
    all_sent(send_sem.at[0], s_ref.at[0:248])
    all_sent(send_sem.at[1], s_ref.at[0:248])
    all_sent(send_sem.at[2], lt.at[0:7])
    all_sent(send_sem.at[3], xv.at[0])
    s_sent()
    t_sent()
    shares_sent()

    def relay(order, onward):
        for q in order:
            up[q].wait_recv()
            if q in onward:
                onward[q].start()
            over[q].start()

    @pl.when(y == 1)
    def _():
        relay((0, 1, 2, 3), {0: up[0], 1: up[1]})

    @pl.when(y == 3)
    def _():
        relay((2, 3, 0, 1), {2: down[2], 3: down[3]})

    @pl.when(y == 2)
    def _():
        relay((0, 2, 1, 3), {})

    def share(which, d):
        rows = pl.ds(pl.multiple_of(which * BS, BS), BS)
        return mm3(halves(yb[which]), (rh[d, rows], rl[d, rows]))

    for d in range(4):
        cut = slice(d * BS, (d + 1) * BS)
        o_ref[:, cut] = o_ref[:, cut] - share(c, d)

    @pl.when((y != 0) | (c == 0))
    def _():
        for e in over:
            e.wait_recv()

    def right(d):
        return o_ref[:, d * BS : (d + 1) * BS] - share(1 - c, d)

    for d in (1, 2, 3):
        write(d, right(d))

    @pl.when(y == 0)
    def _():
        write(0, yb[c])

    @pl.when(y != 0)
    def _():
        write(0, right(0))

    for e in over:
        e.wait_send()

    @pl.when((y == 0) | (y == 1))
    def _():
        up[0].wait_send()
        up[1].wait_send()

    @pl.when((y == 0) | (y == 3))
    def _():
        down[2].wait_send()
        down[3].wait_send()

    @pl.when(y == 0)
    def _():
        for e in (up[2], up[3], down[0], down[1]):
            e.wait_send()


N_EVENTS = 70


def shards(cross_cov, left_factor, right_factor):
    f32 = jnp.float32
    out = pl.pallas_call(
        kernel,
        out_shape=jax.ShapeDtypeStruct((BS * 8, 128), f32),
        in_specs=[
            pl.BlockSpec(memory_space=pltpu.HBM),
            pl.BlockSpec(memory_space=pltpu.HBM),
            pl.BlockSpec(memory_space=pltpu.HBM),
        ],
        out_specs=pl.BlockSpec(memory_space=pltpu.VMEM),
        scratch_shapes=[
            pltpu.VMEM((BS, 1024), f32),
            pltpu.VMEM((BS, 1024), f32),
            pltpu.VMEM((NZ, NX, 4, 16, BS), f32),
            pltpu.VMEM((4, 8, 64, BS), f32),
            pltpu.VMEM((8, 2, 64, BS), f32),
            pltpu.VMEM((8, 64, 256), f32),
            pltpu.VMEM((2, BS, BS), f32),
            pltpu.VMEM((2, BS, BS), f32),
            pltpu.VMEM((4, 2 * BS, BS), jnp.bfloat16),
            pltpu.VMEM((4, 2 * BS, BS), jnp.bfloat16),
            pltpu.SemaphoreType.DMA((3,)),
            pltpu.SemaphoreType.DMA((4,)),
            pltpu.SemaphoreType.DMA((N_EVENTS,)),
            pltpu.SemaphoreType.DMA((1,)),
            pltpu.SemaphoreType.DMA((5,)),
            pltpu.SemaphoreType.DMA((3, 8)),
            pltpu.SemaphoreType.DMA((5,)),
            pltpu.SemaphoreType.DMA((13,)),
            pltpu.SemaphoreType.DMA((12,)),
            pltpu.SemaphoreType.DMA((8,)),
        ],
        compiler_params=pltpu.CompilerParams(collective_id=0, has_side_effects=True, vmem_limit_bytes=55000000),
    )(
        cross_cov.reshape(BS, 8, 128),
        left_factor.reshape(BS, 64).T,
        jnp.swapaxes(right_factor.reshape(4, BS, 16), 1, 2),
    )
    return out.reshape(cross_cov.shape)


def solution(mesh):
    return jax.shard_map(
        shards,
        mesh=mesh,
        in_specs=(
            P(None, "prow", None, None, "pcol", None),
            P(None, "prow", None, "pcol"),
            P(None, "pcol", None, "prow"),
        ),
        out_specs=P(None, "prow", None, None, "pcol", None),
        check_vma=False,
    )
```
